32 devices in a mesh: gx: 8 (over z, core), gy: 4 (over y, x).
Axes of the slice: x: 2, y: 2, z: 4, core: 2. Of those that a mesh axis runs over, the one named last changes fastest.
Arguments:
- mass: float32 [5, 256, 1024], P(None, 'gy', 'gx'), may hold values from 0.05 to 1
- tracer: float32 [5, 7, 256, 1024], P(None, None, 'gy', 'gx'), may hold values from -4 to 4
- uvel: float32 [256, 1024], P('gy', 'gx'), may hold values from -0.45 to 0.45
- vvel: float32 [256, 1024], P('gy', 'gx'), may hold values from -0.45 to 0.45
- case_east: int32 [256, 1024], P('gy', 'gx'), may hold values from 0 to 2
- case_north: int32 [256, 1024], P('gy', 'gx'), may hold values from 0 to 2
- ice_blocks: int32 [8, 32], P('gy', 'gx'), may hold values 0 or 1
Outputs:
- mass_out: float32 [5, 256, 1024], P(None, 'gy', 'gx')
- tracer_out: float32 [5, 7, 256, 1024], P(None, None, 'gy', 'gx')
The draws below stay inside these ranges and needn't reach their ends.
Inputs may be any that keep to these rules, and one draw needn't show every extreme that they name: `case_east`: 0 means no corner triangle, 1 the lower corner, 2 the upper corner. `case_north`: 0 means no corner triangle, 1 the western corner, 2 the eastern corner.
All inputs are finite; a program needn't handle non-finite values. No bound on the sum of `ice_blocks` on one device may be relied on, other than what follows from the above.
Results may differ from the reference program's by a relative error of at most 0.0003.
Values sent between devices are 32-bit elements; how exact they have to be, the bound alone decides.
No kernel may reach another device: no remote copies, remote signals or barrier semaphores. Data moves between devices by JAX's collectives and lax.ppermute only.
A program may use at most 128 MiB of HBM per device.

```python
import jax
import jax.numpy as jnp
from jax import lax

NCAT = 5
NTRC = 7
BS = 32
STEPS = 2
NX = 1024
NY = 256


def place_ends(values, own_key, least, top_value):
    dims = values.shape
    place = [jax.random.randint(jax.random.fold_in(own_key, axis), (), 0, dims[axis]) for axis in range(len(dims))]
    values = values.at[tuple(place)].set(least)
    longest = dims.index(max(dims))
    place[longest] = (place[longest] + 1) % dims[longest]
    return values.at[tuple(place)].set(top_value)


def levels(own_key, shape, pieces, least, largest):
    level = 1.0
    for dim, blocks in pieces:
        heights = jax.random.uniform(jax.random.fold_in(jax.random.fold_in(own_key, 6), dim), (blocks,), jnp.float32, least / len(pieces), largest / len(pieces))
        level = level * jnp.repeat(jnp.exp(heights), shape[dim] // blocks).reshape((-1,) + (1,) * (len(shape) - 1 - dim))
    return level


def scatter_about(key, shape, deviation, bound, cuts=(), dtype=jnp.bfloat16):
    entries = deviation * jax.random.normal(key, shape, jnp.float32)
    if cuts:
        entries = entries * levels(key, shape, cuts, -0.22, 0.18)
    return jnp.clip(entries, -bound, bound).astype(dtype)


def setup_inputs(seed: int = 0) -> dict:
    arg_keys = jax.random.split(jax.random.key(seed), 8)
    mass = jnp.clip(0.05 + 0.95 * jax.random.uniform(arg_keys[0], (NCAT, NY, NX), jnp.float32) ** levels(arg_keys[0], (NCAT, NY, NX), ((1, 4), (2, 8)), -0.2, 0.2), 0.05, 1.0)
    tracer = scatter_about(arg_keys[1], (NCAT, NTRC, NY, NX), 1.0, 4.0, ((2, 4), (3, 8)), jnp.float32)
    uvel = jnp.clip(jax.random.uniform(arg_keys[2], (NY, NX), jnp.float32, -0.45, 0.45) * levels(arg_keys[2], (NY, NX), ((0, 4), (1, 8)), -0.4, 0.0), -0.45, 0.45)
    vvel = jnp.clip(jax.random.uniform(arg_keys[3], (NY, NX), jnp.float32, -0.45, 0.45) * levels(arg_keys[3], (NY, NX), ((0, 4), (1, 8)), -0.4, 0.0), -0.45, 0.45)
    case_east = place_ends(jax.random.randint(arg_keys[4], (NY, NX), 0, 3), jax.random.fold_in(arg_keys[4], 1), 0, 2).astype(jnp.int32)
    case_north = place_ends(jax.random.randint(arg_keys[5], (NY, NX), 0, 3), jax.random.fold_in(arg_keys[5], 1), 0, 2).astype(jnp.int32)
    ice_blocks = place_ends((jax.random.randint(arg_keys[6], (NY // BS, NX // BS), 0, 4) < 3).astype(jnp.int32), jax.random.fold_in(arg_keys[6], 1), 0, 1)
    return dict(mass=mass, tracer=tracer, uvel=uvel, vvel=vvel, case_east=case_east, case_north=case_north, ice_blocks=ice_blocks)


mass_floor = 0.1


def region(region_area, normal_pos, trans_pos, cell):
    values, grad_normal, grad_trans = cell
    centre_val = values + grad_normal * normal_pos + grad_trans * trans_pos
    carried = region_area * centre_val[0]
    return jnp.concatenate([carried[None], carried[None] * centre_val[1:]], axis=0)


def choose(forward, when_true, when_false):
    return tuple(jnp.where(forward, left_arr, right_arr) for left_arr, right_arr in zip(when_true, when_false))


def edge_flux(normal_speed, low_speed, high_speed, case_id, low_side, high_side, low_below, low_above, high_below, high_above):
    forward = normal_speed > 0.0
    signs = jnp.where(forward, 1.0, -1.0)
    reach = jnp.abs(normal_speed)
    source = choose(forward, low_side, high_side)
    beneath = choose(forward, low_below, high_below)
    overhead = choose(forward, low_above, high_above)
    summed = region(reach, signs * (0.5 - 0.5 * reach), 0.0, source)
    tri_normal = signs * (0.5 - reach / 3.0)
    low_area = jnp.where(case_id == 1, 0.5 * reach * low_speed, 0.0)
    low_offset = 0.5 - low_speed / 3.0
    summed = summed + region(low_area, tri_normal, low_offset, beneath) - region(low_area, tri_normal, -low_offset, source)
    high_area = jnp.where(case_id == 2, 0.5 * reach * high_speed, 0.0)
    high_offset = 0.5 - high_speed / 3.0
    summed = summed + region(high_area, tri_normal, -high_offset, overhead) - region(high_area, tri_normal, high_offset, source)
    return signs * summed


def category_fluxes(values, slopes, u_ext, v_ext, case_east_al, case_north_al, east_from, north_from):
    height = values.shape[1] - 2
    breadth = values.shape[2] - 2

    def along_x(row_sel, col_sel):
        return (values[:, row_sel, col_sel], slopes[0][:, row_sel, col_sel], slopes[1][:, row_sel, col_sel])

    def along_y(row_sel, col_sel):
        return (values[:, row_sel, col_sel], slopes[1][:, row_sel, col_sel], slopes[0][:, row_sel, col_sel])

    low_cols = slice(east_from + 1, breadth + 1)
    high_cols = slice(east_from + 2, breadth + 2)
    centre = slice(1, height + 1)
    below_rows = slice(0, height)
    above_rows = slice(2, height + 2)
    speed_east = 0.5 * (u_ext[centre, low_cols] + u_ext[below_rows, low_cols])
    east_flux = edge_flux(speed_east, jnp.abs(v_ext[below_rows, low_cols]), jnp.abs(v_ext[centre, low_cols]), case_east_al,
                          along_x(centre, low_cols), along_x(centre, high_cols), along_x(below_rows, low_cols),
                          along_x(above_rows, low_cols), along_x(below_rows, high_cols), along_x(above_rows, high_cols))
    low_rows = slice(north_from + 1, height + 1)
    high_rows = slice(north_from + 2, height + 2)
    centre_cols = slice(1, breadth + 1)
    west_cols = slice(0, breadth)
    east_cols = slice(2, breadth + 2)
    speed_north = 0.5 * (v_ext[low_rows, centre_cols] + v_ext[low_rows, west_cols])
    north_flux = edge_flux(speed_north, jnp.abs(u_ext[low_rows, west_cols]), jnp.abs(u_ext[low_rows, centre_cols]), case_north_al,
                           along_y(low_rows, centre_cols), along_y(high_rows, centre_cols), along_y(low_rows, west_cols),
                           along_y(low_rows, east_cols), along_y(high_rows, west_cols), along_y(high_rows, east_cols))
    return east_flux, north_flux


def all_fluxes(values, slopes, u_ext, v_ext, case_east_al, case_north_al, east_from, north_from):
    def per_category(paired):
        return category_fluxes(paired[0], paired[1], u_ext, v_ext, case_east_al, case_north_al, east_from, north_from)

    return lax.map(per_category, (values, slopes))


def slope_pair(extended):
    along_lon = 0.5 * (extended[..., 1:-1, 2:] - extended[..., 1:-1, :-2])
    along_lat = 0.5 * (extended[..., 2:, 1:-1] - extended[..., :-2, 1:-1])
    return jnp.stack([along_lon, along_lat], axis=1)


def update(fields, east_flux, north_flux):
    carried = fields[:, 0]
    conserved = jnp.concatenate([carried[:, None], carried[:, None] * fields[:, 1:]], axis=1)
    conserved = conserved - (east_flux[..., 1:] - east_flux[..., :-1]) - (north_flux[..., 1:, :] - north_flux[..., :-1, :])
    new_mass = conserved[:, 0]
    amounts = conserved[:, 1:] / jnp.maximum(new_mass, mass_floor)[:, None]
    return jnp.concatenate([new_mass[:, None], amounts], axis=1)


def extend(source_arr, margin):
    wrapped = jnp.concatenate([source_arr[..., -margin:], source_arr, source_arr[..., :margin]], axis=-1)
    folded = wrapped[..., ::-1, ::-1][..., :margin, :]
    bottom_rows = jnp.zeros(wrapped.shape[:-2] + (margin, wrapped.shape[-1]), jnp.float32)
    return jnp.concatenate([bottom_rows, wrapped, folded], axis=-2)


def reference(mass, tracer, uvel, vvel, case_east, case_north, ice_blocks):
    cell_mask = jnp.repeat(jnp.repeat(ice_blocks, BS, axis=0), BS, axis=1).astype(jnp.float32)
    fields = jnp.concatenate([(mass * cell_mask)[:, None], tracer], axis=1)
    u_ext = jnp.pad(jnp.concatenate([uvel[:, -1:], uvel, uvel[:, :1]], axis=1), ((1, 1), (0, 0)))
    v_ext = jnp.pad(jnp.concatenate([vvel[:, -1:], vvel, vvel[:, :1]], axis=1), ((1, 1), (0, 0)))
    case_east_al = jnp.concatenate([case_east[:, -1:], case_east], axis=1)
    case_north_al = jnp.concatenate([jnp.zeros((1, NX), jnp.int32), case_north], axis=0)
    for sweep in range(STEPS):
        extended = extend(fields, 2)
        slopes = slope_pair(extended)
        east_flux, north_flux = all_fluxes(extended[..., 1:-1, 1:-1], slopes, u_ext, v_ext, case_east_al, case_north_al, -1, -1)
        fields = update(fields, east_flux, north_flux)
    return fields[:, 0], fields[:, 1:]
```

```python
import functools

import jax
import jax.numpy as jnp
from jax import lax
from jax.experimental import pallas as pl
from jax.experimental.pallas import tpu as pltpu
from jax.sharding import PartitionSpec as P

STEPS = 2
MASS_FLOOR = 0.1
PAD = 8
DEPTH = 2 * STEPS
STRIP = 6 * DEPTH
PER_PACK = STRIP // DEPTH
F32 = jnp.float32


def lanes_iota():
    return lax.broadcasted_iota(jnp.int32, (8, 128), 1)


def rows_iota():
    return lax.broadcasted_iota(jnp.int32, (8, 128), 0)


def roll(x, shift):
    return pltpu.roll(x, shift % 128 if isinstance(shift, int) else shift, 1)


def sel(mask, a, b):
    return jnp.where(mask, a, b)


def edge_geometry(speed, low, high, case):
    first = case == 1.0
    corner = sel(first, low, high)
    signs = sel(speed > 0.0, 1.0, -1.0)
    signed_area = sel(case == 0.0, 0.0, 0.5 * speed * corner)
    near = 0.25 * (signs - speed)
    far = 0.25 * signs - speed * (1.0 / 6.0)
    off = 0.25 - corner * (1.0 / 6.0)
    return speed, signed_area, near, far, off, sel(first, off, -off), case


def east_geometry(u, u_below, v, v_below, case):
    return edge_geometry(0.5 * (u + u_below), jnp.abs(v_below), jnp.abs(v), case)


def north_geometry(u, v, case):
    u_west, v_west = roll(u, 1), roll(v, 1)
    return edge_geometry(0.5 * (v + v_west), jnp.abs(u_west), jnp.abs(u), case)


def fill_geometry(geo, tiles, aux):
    for r in tiles:
        u, v = aux(0, r), aux(1, r)
        east = east_geometry(u, aux(0, r - 1), v, aux(1, r - 1), aux(2, r))
        north = north_geometry(u, v, aux(3, r))
        for n in range(7):
            geo[0, n, pl.ds(r, 8), :] = east[n]
            geo[1, n, pl.ds(r, 8), :] = north[n]


def ghost_aux(dst, src, base, top, height):
    for r in (height - 8, height):
        at_fold = jnp.logical_and(top == 1, rows_iota() + r >= height - 1)
        for plane in range(4):
            plain = src(plane, r)
            if plane < 2:
                ghost = -roll(src(plane, r + 1), -1)
            else:
                raw = roll(src(2, r), -1) if plane == 2 else src(3, r + 1)
                ghost = sel(raw == 0.0, 0.0, 3.0 - raw)
            dst[plane, pl.ds(r - base, 8), :] = sel(at_fold, ghost, plain)


def picks(low, high, low_slope, high_slope, forward, first):
    centre = sel(forward, low(0), high(0))
    slope = sel(forward, low_slope(0), high_slope(0))
    before = sel(forward, low(-1), high(-1))
    after = sel(forward, low(1), high(1))
    other_slope = sel(
        forward,
        sel(first, low_slope(-1), low_slope(1)),
        sel(first, high_slope(-1), high_slope(1)),
    )
    beyond = sel(forward, sel(first, low(-2), low(2)), sel(first, high(-2), high(2)))
    return centre, slope, before, after, other_slope, beyond


def fluxes(geo, load, direction, forward=None):
    speed, area, near, far, off, side, case = geo
    forward = speed > 0.0
    first = case == 1.0

    def picked(k):
        memo = {}

        def at(col, row):
            if (col, row) not in memo:
                memo[col, row] = load(k, col, row)
            return memo[col, row]

        if direction == 0:
            return picks(
                lambda d: at(0, d),
                lambda d: at(1, d),
                lambda d: at(1, d) - at(-1, d),
                lambda d: at(2, d) - at(0, d),
                forward,
                first,
            )
        return picks(
            lambda d: at(d, 0),
            lambda d: at(d, 1),
            lambda d: at(d, 1) - at(d, -1),
            lambda d: at(d, 2) - at(d, 0),
            forward,
            first,
        )

    centre, slope, before, after, other_slope, beyond = picked(0)
    other = sel(first, before, after)
    w0 = speed * (centre + near * slope)
    w1 = area * (other + far * other_slope + off * (centre - beyond))
    w2 = area * (centre + far * slope + side * (before - after))
    total = w0 + w1 - w2
    w1_off = w1 * off
    w2_side = w2 * side
    k_centre = w0 - w2 + w1_off
    k_slope = w0 * near - w2 * far
    k_before = sel(first, w1, 0.0) - w2_side
    k_after = sel(first, 0.0, w1) + w2_side
    k_other = w1 * far
    out = [total]
    for k in range(1, 8):
        centre, slope, before, after, other_slope, beyond = picked(k)
        out.append(
            (k_centre * centre + k_slope * slope)
            + (k_before * before + k_after * after)
            + (k_other * other_slope - w1_off * beyond)
        )
    return out


def advance(source, geo, geo_base, first_row, tiles, shifted, north, store):
    low = first_row - 2
    count = 8 * tiles
    starts = [8 * t for t in range(tiles)] + [count - 4]
    for k in range(8):
        for s in starts:
            value = source(k, low + s)
            for n, col in enumerate((1, -1, 2, -2)):
                shifted[n, k, pl.ds(s, 8), :] = roll(value, -col)
    slot = {1: 0, -1: 1, 2: 2, -2: 3}

    def loader(row):
        def load(k, col, shift):
            if col == 0:
                return source(k, row + shift)
            return shifted[slot[col], k, pl.ds(row + shift - low, 8), :]

        return load

    def geometry(direction, row):
        return [geo[direction, n, pl.ds(row + geo_base, 8), :] for n in range(7)]

    def run_north(row):
        flux = fluxes(geometry(1, row), loader(row), 1)
        for k in range(8):
            north[k, pl.ds(row - first_row + 1, 8), :] = flux[k]

    run_north(first_row - 1)
    for t in range(tiles):
        row = first_row + 8 * t
        run_north(row + 7 if t < tiles - 1 else row)
        east = fluxes(geometry(0, row), loader(row), 0)
        mass = source(0, row)

        def conserved(k, carried):
            return (
                carried
                - (east[k] - roll(east[k], 1))
                - (north[k, pl.ds(8 * t + 1, 8), :] - north[k, pl.ds(8 * t, 8), :])
            )

        new_mass = conserved(0, mass)
        store(0, row, new_mass)
        scale = 1.0 / jnp.maximum(new_mass, MASS_FLOOR)
        for k in range(1, 8):
            store(k, row, conserved(k, mass * source(k, row)) * scale)


def block_mask(ice, row, height, width):
    block_rows, block_cols = ice.shape
    lane = lax.broadcasted_iota(jnp.int32, (1, width), 1)
    line = jnp.zeros((1, width), F32)
    which = row // (height // block_rows)
    for b in range(block_cols):
        inside = lane >= b * (width // block_cols)
        line = sel(inside, ice[which, b].astype(F32), line)
    return line


def pack_rows_kernel(place, ice, mass, tracer, u, v, ce, cn, pay_a, pay_b):
    ncat, height, width = mass.shape
    ncomp = tracer.shape[1] + 1

    def rows_of(p, row):
        if p < ncat * ncomp:
            c, k = divmod(p, ncomp)
            if k == 0:
                return mass[c, pl.ds(row, DEPTH), :] * block_mask(ice, row, height, width)
            return tracer[c, k - 1, pl.ds(row, DEPTH), :]
        ref = (u, v, ce, cn)[p - ncat * ncomp]
        return ref[pl.ds(row, DEPTH), :].astype(F32)

    def write(dst, top):
        for p in range(ncat * ncomp + 4):
            half = (p % 2) ^ (1 if top else 0)
            dst[p // 2, pl.ds(DEPTH * half, DEPTH), :] = rows_of(p, height - DEPTH if top else 0)

    @pl.when(place[0] == 0)
    def _():
        write(pay_a, True)
        write(pay_b, False)

    @pl.when(place[0] == 1)
    def _():
        write(pay_a, False)
        write(pay_b, True)


def inner_kernel(ice, mass, tracer, u, v, ce, cn, once, twice, strips, aux, geo, masked, shifted, north):
    ncat, height, width = mass.shape
    lane = lanes_iota()
    for plane, ref in enumerate((u, v, ce, cn)):
        for t in range(0, height, 8):
            aux[plane, pl.ds(t + PAD, 8), :] = ref[pl.ds(t, 8), :].astype(F32)
    fill_geometry(geo, range(PAD, PAD + height, 8), lambda n, r: aux[n, pl.ds(r, 8), :])
    for plane in range(4):
        for t in range(0, height, 8):
            value = aux[plane, pl.ds(t + PAD, 8), :]
            packed = jnp.zeros((8, 128), F32)
            for c in range(ncat):
                packed = strip_place(packed, value, c * STRIP, lane)
            strips[8 + plane, pl.ds(t + PAD, 8), :] = packed

    def category(c, carry):
        for t in range(0, height, 8):
            masked[pl.ds(t, 8), :] = mass[c, pl.ds(t, 8), :] * block_mask(ice, t, height, width)

        def source(k, row):
            if k == 0:
                return masked[pl.ds(row, 8), :]
            return tracer[c, k - 1, pl.ds(row, 8), :]

        def middle(k, row):
            return once[c, k, pl.ds(row + PAD, 8), :]

        def keep_once(k, row, value):
            once[c, k, pl.ds(row + PAD, 8), :] = value

        def keep_twice(k, row, value):
            twice[c, k, pl.ds(row, 8), :] = value

        advance(source, geo, PAD, 6, height // 8 - 1, shifted, north, keep_once)
        advance(middle, geo, PAD, 8, height // 8 - 2, shifted, north, keep_twice)
        for k in range(8):
            for t in range(0, height, 8):
                old = strips[k, pl.ds(t + PAD, 8), :]
                strips[k, pl.ds(t + PAD, 8), :] = strip_place(old, source(k, t), c * STRIP, lane)
        return carry

    lax.fori_loop(0, ncat, category, 0)


def strip_place(packed, value, start, lane):
    low = roll(value, start + DEPTH)
    high = roll(value, start + 5 * DEPTH)
    at = lane - start
    packed = sel(jnp.logical_and(at >= DEPTH, at < 3 * DEPTH), low, packed)
    return sel(jnp.logical_and(at >= 3 * DEPTH, at < 5 * DEPTH), high, packed)


def pack_columns_kernel(place, got_a, got_b, strips_in, halo, strips, pay_w, pay_e, tmp, flip):
    height = strips.shape[1] - 3 * PAD
    lane = lanes_iota()
    even = place[0] == 0
    pairs = got_a.shape[0]
    for q in range(pairs):
        tmp[0, q] = sel(even, got_b[q], got_a[q])
        tmp[1, q] = sel(even, got_a[q], got_b[q])

    @pl.when(place[1] == 1)
    def _():
        for q in range(pairs):
            flip[q] = jnp.take_along_axis(tmp[1, q], 127 - lane, axis=1)
        for q in range(pairs):
            for s in range(8):
                tmp[1, q, pl.ds(s, 1), :] = flip[q, pl.ds(7 - s, 1), :]

    for p in range(2 * pairs):
        half = p % 2
        halo[p, pl.ds(PAD - DEPTH, DEPTH), :] = tmp[0, p // 2, pl.ds(DEPTH * (1 - half), DEPTH), :]
        halo[p, pl.ds(PAD, DEPTH), :] = tmp[1, p // 2, pl.ds(DEPTH * half, DEPTH), :]
    ncat = (2 * pairs - 4) // 8
    for k in range(12):
        for side in range(2):
            packed = jnp.zeros((8, 128), F32)
            for c in range(ncat):
                p = 8 * c + k if k < 8 else 8 * ncat + k - 8
                packed = strip_place(packed, halo[p, pl.ds(8 * side, 8), :], c * STRIP, lane)
            strips[k, pl.ds(side * (height + PAD), 8), :] = packed
    where = lax.rem(lane, STRIP) // DEPTH
    for g in range(2):
        for t in range(0, height + 2 * DEPTH, 8):
            west = jnp.zeros((8, 128), F32)
            east = jnp.zeros((8, 128), F32)
            for n in range(PER_PACK):
                value = strips[PER_PACK * g + n, pl.ds(t + PAD - DEPTH, 8), :]
                west = sel(where == n, roll(value, DEPTH * (n - 1)), west)
                east = sel(where == n, roll(value, DEPTH * (n - 4)), east)
            pay_w[g, pl.ds(t, 8), :] = west
            pay_e[g, pl.ds(t, 8), :] = east


def rim_kernel(place, ice, mass, tracer, u, v, ce, cn, once, halo, rim, aux, ghost, geo, geo_ghost, field, stage, shifted, north, spare):
    ncat, height, width = mass.shape
    own = ncat * 8
    top = place[1]
    for plane, ref in enumerate((u, v, ce, cn)):
        aux[0, plane, pl.ds(0, 8), :] = halo[own + plane, pl.ds(0, 8), :]
        for n in range(2):
            aux[0, plane, pl.ds(8 + 8 * n, 8), :] = ref[pl.ds(8 * n, 8), :].astype(F32)
            aux[1, plane, pl.ds(8 * n, 8), :] = ref[pl.ds(height - 16 + 8 * n, 8), :].astype(F32)
        aux[1, plane, pl.ds(16, 8), :] = halo[own + plane, pl.ds(8, 8), :]
    ghost_aux(ghost, lambda n, r: aux[1, n, pl.ds(r - height + 16, 8), :], height - 16, top, height)
    for plane in range(4):
        ghost[plane, pl.ds(0, 8), :] = aux[1, plane, pl.ds(0, 8), :]
    fill_geometry(geo.at[0], (PAD - 3, PAD, PAD + 8), lambda n, r: aux[0, n, pl.ds(r, 8), :])
    fill_geometry(geo.at[1], (1, 8, 16), lambda n, r: aux[1, n, pl.ds(r, 8), :])
    fill_geometry(geo_ghost, (8, 16), lambda n, r: ghost[n, pl.ds(r, 8), :])
    above = rows_iota() >= 2

    def category(c, carry):
        field[0, 0, pl.ds(8, 8), :] = mass[c, pl.ds(0, 8), :] * block_mask(ice, 0, height, width)
        field[1, 0, pl.ds(0, 8), :] = mass[c, pl.ds(height - 8, 8), :] * block_mask(
            ice, height - 8, height, width
        )
        for k in range(8):
            field[0, k, pl.ds(0, 8), :] = halo[8 * c + k, pl.ds(0, 8), :]
            field[1, k, pl.ds(8, 8), :] = halo[8 * c + k, pl.ds(8, 8), :]
            if k:
                field[0, k, pl.ds(8, 8), :] = tracer[c, k - 1, pl.ds(0, 8), :]
                field[1, k, pl.ds(0, 8), :] = tracer[c, k - 1, pl.ds(height - 8, 8), :]
            stage[0, k, pl.ds(14, 8), :] = once[c, k, pl.ds(6 + PAD, 8), :]
            stage[1, k, pl.ds(6, 8), :] = once[c, k, pl.ds(height - 10 + PAD, 8), :]

        def low_field(k, row):
            return field[0, k, pl.ds(row + 8, 8), :]

        def high_field(k, row):
            return field[1, k, pl.ds(row - (height - 8), 8), :]

        def keep_low(k, row, value):
            stage[0, k, pl.ds(row + 8, 8), :] = value

        def keep_high(k, row, value):
            stage[1, k, pl.ds(row - (height - 16), 8), :] = value

        def keep_ghost(k, row, value):
            mine = stage[1, k, pl.ds(row - (height - 16), 8), :]
            stage[1, k, pl.ds(row - (height - 16), 8), :] = sel(above, value, mine)

        advance(low_field, geo.at[0], PAD, -2, 1, shifted, north, keep_low)
        advance(high_field, geo.at[1], 16 - height, height - 2, 1, shifted, north, keep_high)
        advance(high_field, geo_ghost, 16 - height, height - 2, 1, shifted, north, keep_ghost)

        def low_stage(k, row):
            return stage[0, k, pl.ds(row + 8, 8), :]

        def high_stage(k, row):
            return stage[1, k, pl.ds(row - (height - 16), 8), :]

        def out_low(k, row, value):
            rim[c, k, pl.ds(0, 8), :] = value

        def out_high(k, row, value):
            rim[c, k, pl.ds(8, 8), :] = value

        advance(low_stage, geo.at[0], PAD, 0, 1, shifted, north, out_low)
        advance(high_stage, geo.at[1], 16 - height, height - 8, 1, shifted, north, out_high)
        return carry

    lax.fori_loop(0, ncat, category, 0)


def finish_kernel(place, strips_in, got_w, got_e, twice, rim, mass_out, tracer_out, strips, ghost, geo, geo_ghost, stage, last, shifted, north):
    ncat, height, width = mass_out.shape
    lane = lanes_iota()
    at = lax.rem(lane, STRIP)
    for k in range(12):
        g, n = divmod(k, PER_PACK)
        for t in range(0, height + 2 * DEPTH, 8):
            value = strips_in[k, pl.ds(t + PAD - DEPTH, 8), :]
            value = sel(at < DEPTH, roll(got_w[g, pl.ds(t, 8), :], -DEPTH * n), value)
            value = sel(at >= 5 * DEPTH, roll(got_e[g, pl.ds(t, 8), :], DEPTH * (5 - n)), value)
            strips[k, pl.ds(t + PAD - DEPTH, 8), :] = value

    def aux(n, r):
        return strips[8 + n, pl.ds(r, 8), :]

    ghost_aux(ghost, lambda n, r: aux(n, r + PAD), height - 16, place[1], height)
    for plane in range(4):
        ghost[plane, pl.ds(0, 8), :] = aux(plane, height - 16 + PAD)
    fill_geometry(geo, [PAD - 3] + list(range(PAD, PAD + height + 1, 8)), aux)
    fill_geometry(geo_ghost, (8, 16), lambda n, r: ghost[n, pl.ds(r, 8), :])
    above = rows_iota() >= 2

    def source(k, row):
        return strips[k, pl.ds(row + PAD, 8), :]

    def keep(k, row, value):
        stage[k, pl.ds(row + PAD, 8), :] = value

    def keep_ghost(k, row, value):
        stage[k, pl.ds(row + PAD, 8), :] = sel(above, value, stage[k, pl.ds(row + PAD, 8), :])

    def middle(k, row):
        return stage[k, pl.ds(row + PAD, 8), :]

    def keep_last(k, row, value):
        last[k, pl.ds(row, 8), :] = value

    advance(source, geo, PAD, -2, height // 8 + 1, shifted, north, keep)
    advance(source, geo_ghost, 16 - height, height - 2, 1, shifted, north, keep_ghost)
    advance(middle, geo, PAD, 0, height // 8, shifted, north, keep_last)

    def category(c, carry):
        for k in range(8):
            for t in range(0, height, 8):
                if t == 0:
                    value = rim[c, k, pl.ds(0, 8), :]
                elif t == height - 8:
                    value = rim[c, k, pl.ds(8, 8), :]
                else:
                    value = twice[c, k, pl.ds(t, 8), :]
                edge = last[k, pl.ds(t, 8), :]
                value = sel(lane < DEPTH, roll(edge, 2 * 128 - DEPTH - c * STRIP), value)
                value = sel(lane >= 128 - DEPTH, roll(edge, 128 - 5 * DEPTH + 128 - c * STRIP), value)
                if k == 0:
                    mass_out[c, pl.ds(t, 8), :] = value
                else:
                    tracer_out[c, k - 1, pl.ds(t, 8), :] = value
        return carry

    lax.fori_loop(0, ncat, category, 0)


def shape(*dims):
    return jax.ShapeDtypeStruct(dims, F32)


VMEM = pl.BlockSpec(memory_space=pltpu.VMEM)
SMEM = pl.BlockSpec(memory_space=pltpu.SMEM)


def call(kernel, n_smem, args, outs, scratch, flops, aliases=None, limit=24):
    return pl.pallas_call(
        kernel,
        out_shape=outs,
        in_specs=[SMEM] * n_smem + [VMEM] * (len(args) - n_smem),
        out_specs=jax.tree.map(lambda _: VMEM, outs),
        scratch_shapes=[pltpu.VMEM(dims, F32) for dims in scratch],
        input_output_aliases=aliases or {},
        compiler_params=pltpu.CompilerParams(vmem_limit_bytes=limit << 20),
        cost_estimate=pl.CostEstimate(flops=flops, bytes_accessed=1 << 16, transcendentals=0),
        name=kernel.__name__,
    )(*args)


def per_device(mass, tracer, uvel, vvel, case_east, case_north, ice_blocks):
    ncat, height, width = mass.shape
    ncomp = tracer.shape[1] + 1
    nx, ny = lax.axis_size("gx"), lax.axis_size("gy")
    my_y = lax.axis_index("gy")
    place = jnp.stack([my_y % 2, (my_y == ny - 1).astype(jnp.int32)]).astype(jnp.int32)
    local = (mass, tracer, uvel, vvel, case_east, case_north)
    pairs = (ncat * ncomp + 4) // 2
    rows = height + 2 * PAD

    pay_a, pay_b = call(
        pack_rows_kernel, 2, (place, ice_blocks) + local, (shape(pairs, 8, width),) * 2, [], 1 << 20
    )
    both = ("gx", "gy")
    pairs_a, pairs_b = [], []
    for j in range(ny):
        for i in range(nx):
            pairs_a.append((i * ny + j, i * ny + (j ^ 1)))
            if j == ny - 1:
                pairs_b.append((i * ny + j, (nx - 1 - i) * ny + j))
            elif j:
                pairs_b.append((i * ny + j, i * ny + (j + 1 if j % 2 else j - 1)))
    got_a = lax.ppermute(pay_a, both, pairs_a)
    got_b = lax.ppermute(pay_b, both, pairs_b)

    once, twice, strips = call(
        inner_kernel,
        1,
        (ice_blocks,) + local,
        (shape(ncat, 8, rows, width), shape(ncat, 8, height, width), shape(12, rows + PAD, width)),
        [
            (4, rows, width),
            (2, 7, rows, width),
            (height, width),
            (4, 8, rows, width),
            (8, rows, width),
        ],
        1 << 27,
    )
    halo, strips, pay_w, pay_e = call(
        pack_columns_kernel,
        1,
        (place, got_a, got_b, strips),
        (
            shape(2 * pairs, 16, width),
            shape(12, rows + PAD, width),
            shape(2, height + 2 * DEPTH, width),
            shape(2, height + 2 * DEPTH, width),
        ),
        [(2, pairs, 8, width), (pairs, 8, width)],
        1 << 20,
        aliases={3: 1},
    )
    ahead = [(i, (i + 1) % nx) for i in range(nx)]
    back = [(target, source) for source, target in ahead]
    got_w = lax.ppermute(pay_e, "gx", ahead)
    got_e = lax.ppermute(pay_w, "gx", back)
    (rim,) = call(
        rim_kernel,
        2,
        (place, ice_blocks) + local + (once, halo),
        (shape(ncat, 8, 16, width),),
        [
            (2, 4, 40, width),
            (4, 40, width),
            (2, 2, 7, 40, width),
            (2, 7, 40, width),
            (2, 8, 24, width),
            (2, 8, 32, width),
            (4, 8, 24, width),
            (8, 24, width),
            (8, width),
        ],
        1 << 26,
    )
    return call(
        finish_kernel,
        1,
        (place, strips, got_w, got_e, twice, rim),
        (shape(ncat, height, width), shape(ncat, ncomp - 1, height, width)),
        [
            (12, rows + PAD, width),
            (4, 40, width),
            (2, 7, rows, width),
            (2, 7, 40, width),
            (8, rows, width),
            (8, height, width),
            (4, 8, rows, width),
            (8, rows, width),
        ],
        1 << 26,
    )


def solution(mesh):
    placed = (
        P(None, "gy", "gx"),
        P(None, None, "gy", "gx"),
        P("gy", "gx"),
        P("gy", "gx"),
        P("gy", "gx"),
        P("gy", "gx"),
        P("gy", "gx"),
    )
    return jax.shard_map(
        per_device,
        mesh=mesh,
        in_specs=placed,
        out_specs=(P(None, "gy", "gx"), P(None, None, "gy", "gx")),
        check_vma=False,
    )
```

```python
import functools

import jax
import jax.numpy as jnp
from jax import lax
from jax.experimental import pallas as pl
from jax.experimental.pallas import tpu as pltpu
from jax.sharding import PartitionSpec as P

STEPS = 2
MASS_FLOOR = 0.1
FLAGS = {}
PAD = 8
DEPTH = 2 * STEPS
STRIP = 6 * DEPTH
PER_PACK = STRIP // DEPTH
F32 = jnp.float32


def lanes_iota():
    return lax.broadcasted_iota(jnp.int32, (8, 128), 1)


def rows_iota():
    return lax.broadcasted_iota(jnp.int32, (8, 128), 0)


def roll(x, shift):
    return pltpu.roll(x, shift % 128 if isinstance(shift, int) else shift, 1)


def sel(mask, a, b):
    return jnp.where(mask, a, b)


def edge_geometry(speed, low, high, case):
    first = case == 1.0
    corner = sel(first, low, high)
    signs = sel(speed > 0.0, 1.0, -1.0)
    signed_area = sel(case == 0.0, 0.0, 0.5 * speed * corner)
    near = 0.25 * (signs - speed)
    far = 0.25 * signs - speed * (1.0 / 6.0)
    off = 0.25 - corner * (1.0 / 6.0)
    return speed, signed_area, near, far, off, sel(first, off, -off), case


def east_geometry(u, u_below, v, v_below, case):
    return edge_geometry(0.5 * (u + u_below), jnp.abs(v_below), jnp.abs(v), case)


def north_geometry(u, v, case):
    u_west, v_west = roll(u, 1), roll(v, 1)
    return edge_geometry(0.5 * (v + v_west), jnp.abs(u_west), jnp.abs(u), case)


def fill_geometry(geo, tiles, aux):
    for r in tiles:
        u, v = aux(0, r), aux(1, r)
        east = east_geometry(u, aux(0, r - 1), v, aux(1, r - 1), aux(2, r))
        north = north_geometry(u, v, aux(3, r))
        for n in range(7):
            geo[0, n, pl.ds(r, 8), :] = east[n]
            geo[1, n, pl.ds(r, 8), :] = north[n]


def ghost_aux(dst, src, base, top, height):
    for plane in range(4):
        dst[plane, pl.ds(0, 8), :] = src(plane, base)
    for r in (height - 8, height):
        at_fold = jnp.logical_and(top, rows_iota() + r >= height - 1)
        for plane in range(4):
            plain = src(plane, r)
            if plane < 2:
                ghost = -roll(src(plane, r + 1), -1)
            else:
                raw = roll(src(2, r), -1) if plane == 2 else src(3, r + 1)
                ghost = sel(raw == 0.0, 0.0, 3.0 - raw)
            dst[plane, pl.ds(r - base, 8), :] = sel(at_fold, ghost, plain)


def picks(low, high, low_slope, high_slope, forward, first):
    centre = sel(forward, low(0), high(0))
    slope = sel(forward, low_slope(0), high_slope(0))
    before = sel(forward, low(-1), high(-1))
    after = sel(forward, low(1), high(1))
    other_slope = sel(
        forward,
        sel(first, low_slope(-1), low_slope(1)),
        sel(first, high_slope(-1), high_slope(1)),
    )
    beyond = sel(forward, sel(first, low(-2), low(2)), sel(first, high(-2), high(2)))
    return centre, slope, before, after, other_slope, beyond


class Window:
    def __init__(self, load):
        self.load = load
        self.memo = {}

    def __call__(self, col, row):
        if (col, row) not in self.memo:
            self.memo[col, row] = self.load(col, row)
        return self.memo[col, row]


def picked(at, direction, masks):
    if direction == 0:
        return picks(
            lambda d: at(0, d),
            lambda d: at(1, d),
            lambda d: at(1, d) - at(-1, d),
            lambda d: at(2, d) - at(0, d),
            *masks,
        )
    return picks(
        lambda d: at(d, 0),
        lambda d: at(d, 1),
        lambda d: at(d, 1) - at(d, -1),
        lambda d: at(d, 2) - at(d, 0),
        *masks,
    )


def mass_flux(geo, at, direction):
    speed, area, near, far, off, side, case = geo
    masks = (speed > 0.0, case == 1.0)
    centre, slope, before, after, other_slope, beyond = picked(at, direction, masks)
    first = masks[1]
    other = sel(first, before, after)
    w0 = speed * (centre + near * slope)
    w1 = area * (other + far * other_slope + off * (centre - beyond))
    w2 = area * (centre + far * slope + side * (before - after))
    w1_off = w1 * off
    w2_side = w2 * side
    weights = (
        w0 - w2 + w1_off,
        w0 * near - w2 * far,
        sel(first, w1, 0.0) - w2_side,
        sel(first, 0.0, w1) + w2_side,
        w1 * far,
        w1_off,
    )
    return w0 + w1 - w2, (masks, weights)


def tracer_flux(shared, at, direction):
    masks, weights = shared
    centre, slope, before, after, other_slope, beyond = picked(at, direction, masks)
    return (
        (weights[0] * centre + weights[1] * slope)
        + (weights[2] * before + weights[3] * after)
        + (weights[4] * other_slope - weights[5] * beyond)
    )


def advance(source, geo, geo_base, first_row, tiles, shifted, north, store, south=None):
    low = first_row - 2
    count = 8 * tiles
    starts = [8 * t for t in range(tiles)] + [count - 4]
    for k in range(8):
        for s in starts:
            value = source(k, low + s)
            for n, col in enumerate((1, -1, 2, -2)):
                shifted[n, k, pl.ds(s, 8), :] = roll(value, -col)
    slot = {1: 0, -1: 1, 2: 2, -2: 3}

    def window(k, row):
        def load(col, shift):
            if col == 0:
                return source(k, row + shift)
            return shifted[slot[col], k, pl.ds(row + shift - low, 8), :]

        return Window(load)

    def geometry(direction, row):
        return [geo[direction, n, pl.ds(row + geo_base, 8), :] for n in range(7)]

    def north_alone(row, data):
        at = window(0, row)
        total, shared = mass_flux(data, at, 1)
        out = [total]
        for k in range(1, 8):
            out.append(tracer_flux(shared, window(k, row), 1))
        return out

    if tiles > 1 or south is None:
        below = north_alone(first_row - 1, geometry(1, first_row - 1))
        if tiles > 1:
            for k in range(8):
                north[k, pl.ds(0, 8), :] = below[k]
    for t in range(tiles):
        row = first_row + 8 * t
        if south is not None and t == tiles - 1:
            below = north_alone(row - 1, south)
        elif tiles > 1:
            below = None
        at = window(0, row)
        east_mass, east_shared = mass_flux(geometry(0, row), at, 0)
        north_mass, north_shared = mass_flux(geometry(1, row), at, 1)
        mass = at(0, 0)
        new_mass = None
        for k in range(8):
            if k == 0:
                east, upper, carried = east_mass, north_mass, mass
            else:
                at = window(k, row)
                east = tracer_flux(east_shared, at, 0)
                upper = tracer_flux(north_shared, at, 1)
                carried = mass * at(0, 0)
            if tiles > 1 and t < tiles - 1:
                north[k, pl.ds(8 * t + 1, 8), :] = upper
            elif tiles > 1 and below is None:
                north[k, pl.ds(8 * t + 1, 8), :] = upper
            lower = north[k, pl.ds(8 * t, 8), :] if below is None else below[k]
            fresh = (carried - upper + lower) - (east - roll(east, 1))
            if k == 0:
                scale = 1.0 / jnp.maximum(fresh, MASS_FLOOR)
            else:
                fresh = fresh * scale
            store(k, row, fresh)


def parity():
    return lax.rem(lax.axis_index("gy"), 2)


def at_fold_block():
    return lax.axis_index("gy") == lax.axis_size("gy") - 1


def pack_rows_kernel(ice, mass, tracer, u, v, ce, cn, pay_a, pay_b, mask, ice_s, low, high, low_f, high_f, low_i, high_i, sems):
    ncat, height, width = mass.shape
    ncomp = tracer.shape[1] + 1
    block_rows, block_cols = ice.shape
    copies = [pltpu.make_async_copy(ice, ice_s, sems.at[0])]

    def fetch(src, dst):
        copies.append(pltpu.make_async_copy(src, dst, sems.at[len(copies)]))

    for end, (data, floats, ints) in enumerate(((low, low_f, low_i), (high, high_f, high_i))):
        rows = pl.ds(end * (height - 8), 8)
        fetch(tracer.at[:, :, rows, :], data.at[:, pl.ds(1, ncomp - 1)])
        fetch(mass.at[:, rows, :], data.at[:, 0])
        fetch(u.at[rows, :], floats.at[0])
        fetch(v.at[rows, :], floats.at[1])
        fetch(ce.at[rows, :], ints.at[0])
        fetch(cn.at[rows, :], ints.at[1])
    for copy in copies:
        copy.start()
    for copy in copies:
        copy.wait()
    lane = lanes_iota()
    for b in range(block_rows):
        tile = jnp.zeros((8, width), F32)
        for n in range(block_cols):
            inside = lane >= n * (width // block_cols)
            tile = sel(inside, ice_s[b, n].astype(F32), tile)
        for t in range(height // block_rows // 8):
            mask[pl.ds(b * (height // block_rows) + 8 * t, 8), :] = tile
        if b == 0:
            for c in range(ncat):
                low[c, 0] = low[c, 0] * tile
        if b == block_rows - 1:
            for c in range(ncat):
                high[c, 0] = high[c, 0] * tile

    def write(dst, top):
        data, floats, ints = (high, high_f, high_i) if top else (low, low_f, low_i)
        rows = pl.ds(8 - DEPTH if top else 0, DEPTH)
        for p in range(ncat * ncomp + 4):
            c, k = divmod(p, ncomp)
            if c < ncat:
                value = data[c, k, rows, :]
            elif k < 2:
                value = floats[k, rows, :]
            else:
                value = ints[k - 2, rows, :].astype(F32)
            half = (p % 2) ^ (1 if top else 0)
            dst[p // 2, pl.ds(DEPTH * half, DEPTH), :] = value

    @pl.when(parity() == 0)
    def _():
        write(pay_a, True)
        write(pay_b, False)

    @pl.when(parity() == 1)
    def _():
        write(pay_a, False)
        write(pay_b, True)


def inner_kernel(mask, mass, tracer, u, v, ce, cn, once, twice, strips, aux, geo, masked, shifted, north):
    ncat, height, width = mass.shape
    lane = lanes_iota()
    for plane, ref in enumerate((u, v, ce, cn)):
        for t in range(0, height, 8):
            aux[plane, pl.ds(t + PAD, 8), :] = ref[pl.ds(t, 8), :].astype(F32)
    fill_geometry(geo, range(PAD, PAD + height, 8), lambda n, r: aux[n, pl.ds(r, 8), :])
    for plane in range(4):
        for t in range(0, height, 8):
            value = aux[plane, pl.ds(t + PAD, 8), :]
            packed = jnp.zeros((8, 128), F32)
            for c in range(ncat):
                packed = strip_place(packed, value, c * STRIP, lane)
            strips[8 + plane, pl.ds(t + PAD, 8), :] = packed

    def category(c, carry):
        for t in range(0, height, 8):
            masked[pl.ds(t, 8), :] = mass[c, pl.ds(t, 8), :] * mask[pl.ds(t, 8), :]

        def source(k, row):
            if k == 0:
                return masked[pl.ds(row, 8), :]
            return tracer[c, k - 1, pl.ds(row, 8), :]

        def middle(k, row):
            return once[c, k, pl.ds(row + PAD, 8), :]

        def keep_once(k, row, value):
            once[c, k, pl.ds(row + PAD, 8), :] = value

        def keep_twice(k, row, value):
            twice[c, k, pl.ds(row, 8), :] = value

        advance(source, geo, PAD, 6, height // 8 - 1, shifted, north, keep_once)
        advance(middle, geo, PAD, 8, height // 8 - 2, shifted, north, keep_twice)
        for k in range(8):
            for t in range(0, height, 8):
                old = strips[k, pl.ds(t + PAD, 8), :]
                strips[k, pl.ds(t + PAD, 8), :] = strip_place(old, source(k, t), c * STRIP, lane)
        return carry

    lax.fori_loop(0, ncat, category, 0)


def strip_place(packed, value, start, lane):
    low = roll(value, start + DEPTH)
    high = roll(value, start + 5 * DEPTH)
    at = lane - start
    packed = sel(jnp.logical_and(at >= DEPTH, at < 3 * DEPTH), low, packed)
    return sel(jnp.logical_and(at >= 3 * DEPTH, at < 5 * DEPTH), high, packed)


def pack_columns_kernel(got_a, got_b, strips_in, halo, strips, pay_w, pay_e, tmp, flip):
    height = strips.shape[1] - 3 * PAD
    lane = lanes_iota()
    even = parity() == 0
    pairs = got_a.shape[0]
    for q in range(pairs):
        tmp[0, q] = sel(even, got_b[q], got_a[q])
        tmp[1, q] = sel(even, got_a[q], got_b[q])

    @pl.when(at_fold_block())
    def _():
        for q in range(pairs):
            flip[q] = jnp.take_along_axis(tmp[1, q], 127 - lane, axis=1)
        for q in range(pairs):
            for s in range(8):
                tmp[1, q, pl.ds(s, 1), :] = flip[q, pl.ds(7 - s, 1), :]

    for p in range(2 * pairs):
        half = p % 2
        halo[p, pl.ds(PAD - DEPTH, DEPTH), :] = tmp[0, p // 2, pl.ds(DEPTH * (1 - half), DEPTH), :]
        halo[p, pl.ds(PAD, DEPTH), :] = tmp[1, p // 2, pl.ds(DEPTH * half, DEPTH), :]
    ncat = (2 * pairs - 4) // 8
    for k in range(12):
        for side in range(2):
            packed = jnp.zeros((8, 128), F32)
            for c in range(ncat):
                p = 8 * c + k if k < 8 else 8 * ncat + k - 8
                packed = strip_place(packed, halo[p, pl.ds(8 * side, 8), :], c * STRIP, lane)
            strips[k, pl.ds(side * (height + PAD), 8), :] = packed
    where = lax.rem(lane, STRIP) // DEPTH
    for g in range(2):
        for t in range(0, height + 2 * DEPTH, 8):
            west = jnp.zeros((8, 128), F32)
            east = jnp.zeros((8, 128), F32)
            for n in range(PER_PACK):
                value = strips[PER_PACK * g + n, pl.ds(t + PAD - DEPTH, 8), :]
                west = sel(where == n, roll(value, DEPTH * (n - 1)), west)
                east = sel(where == n, roll(value, DEPTH * (n - 4)), east)
            pay_w[g, pl.ds(t, 8), :] = west
            pay_e[g, pl.ds(t, 8), :] = east


def rim_kernel(mask, mass, tracer, u, v, ce, cn, once, halo, rim, aux, ghost, geo, field, stage, shifted, north):
    ncat, height, width = mass.shape
    own = ncat * 8
    for plane, ref in enumerate((u, v, ce, cn)):
        aux[0, plane, pl.ds(0, 8), :] = halo[own + plane, pl.ds(0, 8), :]
        for n in range(2):
            aux[0, plane, pl.ds(8 + 8 * n, 8), :] = ref[pl.ds(8 * n, 8), :].astype(F32)
            aux[1, plane, pl.ds(8 * n, 8), :] = ref[pl.ds(height - 16 + 8 * n, 8), :].astype(F32)
        aux[1, plane, pl.ds(16, 8), :] = halo[own + plane, pl.ds(8, 8), :]

    def high_aux(n, r):
        return aux[1, n, pl.ds(r - height + 16, 8), :]

    def ghost_rows(n, r):
        return ghost[n, pl.ds(r, 8), :]

    ghost_aux(ghost, high_aux, height - 16, at_fold_block(), height)
    fill_geometry(geo.at[0], (PAD - 3, PAD), lambda n, r: aux[0, n, pl.ds(r, 8), :])
    fill_geometry(geo.at[1], (1, 8), lambda n, r: aux[1, n, pl.ds(r, 8), :])
    fill_geometry(geo.at[1], (16,), ghost_rows)
    south = north_geometry(*(ghost_rows(n, 13) for n in (0, 1, 3)))

    def category(c, carry):
        field[0, 0, pl.ds(8, 8), :] = mass[c, pl.ds(0, 8), :] * mask[pl.ds(0, 8), :]
        field[1, 0, pl.ds(0, 8), :] = mass[c, pl.ds(height - 8, 8), :] * mask[pl.ds(height - 8, 8), :]
        for k in range(8):
            field[0, k, pl.ds(0, 8), :] = halo[8 * c + k, pl.ds(0, 8), :]
            field[1, k, pl.ds(8, 8), :] = halo[8 * c + k, pl.ds(8, 8), :]
            if k:
                field[0, k, pl.ds(8, 8), :] = tracer[c, k - 1, pl.ds(0, 8), :]
                field[1, k, pl.ds(0, 8), :] = tracer[c, k - 1, pl.ds(height - 8, 8), :]
            stage[0, k, pl.ds(14, 8), :] = once[c, k, pl.ds(6 + PAD, 8), :]
            stage[1, k, pl.ds(6, 8), :] = once[c, k, pl.ds(height - 10 + PAD, 8), :]

        def low_field(k, row):
            return field[0, k, pl.ds(row + 8, 8), :]

        def high_field(k, row):
            return field[1, k, pl.ds(row - (height - 8), 8), :]

        def low_stage(k, row):
            return stage[0, k, pl.ds(row + 8, 8), :]

        def high_stage(k, row):
            return stage[1, k, pl.ds(row - (height - 16), 8), :]

        def keep_low(k, row, value):
            stage[0, k, pl.ds(row + 8, 8), :] = value

        def keep_high(k, row, value):
            stage[1, k, pl.ds(row - (height - 16), 8), :] = value

        def out_low(k, row, value):
            rim[c, k, pl.ds(0, 8), :] = value

        def out_high(k, row, value):
            rim[c, k, pl.ds(8, 8), :] = value

        low, high = geo.at[0], geo.at[1]
        up = 16 - height
        advance(low_field, low, PAD, -2, 1, shifted.at[0], north, keep_low)
        advance(high_field, high, up, height - 2, 1, shifted.at[1], north, keep_high, south)
        advance(low_stage, low, PAD, 0, 1, shifted.at[2], north, out_low)
        advance(high_stage, high, up, height - 8, 1, shifted.at[3], north, out_high)
        return carry

    lax.fori_loop(0, ncat, category, 0)


def finish_kernel(strips_in, got_w, got_e, twice, rim, mass_out, tracer_out, strips, ghost, geo, stage, last, shifted, north, whole, sems):
    ncat, height, width = mass_out.shape
    lane = lanes_iota()
    at = lax.rem(lane, STRIP)
    for k in range(12):
        g, n = divmod(k, PER_PACK)
        for t in range(0, height + 2 * DEPTH, 8):
            value = strips_in[k, pl.ds(t + PAD - DEPTH, 8), :]
            value = sel(at < DEPTH, roll(got_w[g, pl.ds(t, 8), :], -DEPTH * n), value)
            value = sel(at >= 5 * DEPTH, roll(got_e[g, pl.ds(t, 8), :], DEPTH * (5 - n)), value)
            strips[k, pl.ds(t + PAD - DEPTH, 8), :] = value

    def aux(n, r):
        return strips[8 + n, pl.ds(r, 8), :]

    def ghost_rows(n, r):
        return ghost[n, pl.ds(r - (height - 16 + PAD), 8), :]

    ghost_aux(ghost, lambda n, r: aux(n, r + PAD), height - 16, at_fold_block(), height)
    fill_geometry(geo, [PAD - 3] + list(range(PAD, PAD + height, 8)), aux)
    fill_geometry(geo, (PAD + height,), ghost_rows)
    south = north_geometry(*(ghost_rows(n, PAD + height - 3) for n in (0, 1, 3)))

    def source(k, row):
        return strips[k, pl.ds(row + PAD, 8), :]

    def keep(k, row, value):
        stage[k, pl.ds(row + PAD, 8), :] = value

    def middle(k, row):
        return stage[k, pl.ds(row + PAD, 8), :]

    def keep_last(k, row, value):
        last[k, pl.ds(row, 8), :] = value

    advance(source, geo, PAD, -2, height // 8 + 1, shifted, north, keep, south)
    advance(middle, geo, PAD, 0, height // 8, shifted, north, keep_last)

    def out_copies(c):
        return (
            pltpu.make_async_copy(whole.at[c, 0], mass_out.at[c], sems.at[0, c]),
            pltpu.make_async_copy(whole.at[c, pl.ds(1, 7)], tracer_out.at[c], sems.at[1, c]),
        )

    def category(c, carry):
        for k in range(8):
            for t in range(0, height, 8):
                if t == 0:
                    value = rim[c, k, pl.ds(0, 8), :]
                elif t == height - 8:
                    value = rim[c, k, pl.ds(8, 8), :]
                else:
                    value = twice[c, k, pl.ds(t, 8), :]
                edge = last[k, pl.ds(t, 8), :]
                value = sel(lane < DEPTH, roll(edge, 2 * 128 - DEPTH - c * STRIP), value)
                value = sel(lane >= 128 - DEPTH, roll(edge, 128 - 5 * DEPTH + 128 - c * STRIP), value)
                whole[c, k, pl.ds(t, 8), :] = value

        @pl.when(c > 0)
        def _():
            for copy in out_copies(c - 1):
                copy.start()

        return carry

    lax.fori_loop(0, ncat, category, 0)
    for copy in out_copies(ncat - 1):
        copy.start()
    for c in range(ncat):
        for copy in out_copies(c):
            copy.wait()


def shape(*dims):
    return jax.ShapeDtypeStruct(dims, F32)


VMEM = pl.BlockSpec(memory_space=pltpu.VMEM)
ANY = pl.BlockSpec(memory_space=pl.ANY)


def call(kernel, args, outs, scratch, flops, aliases=None, specs=None, out_spec=VMEM):
    return pl.pallas_call(
        kernel,
        out_shape=outs,
        in_specs=specs or [VMEM] * len(args),
        out_specs=jax.tree.map(lambda _: out_spec, outs),
        scratch_shapes=[pltpu.VMEM(dims, F32) if isinstance(dims, tuple) else dims for dims in scratch],
        input_output_aliases=aliases or {},
        compiler_params=pltpu.CompilerParams(vmem_limit_bytes=24 << 20, flags=FLAGS),
        cost_estimate=pl.CostEstimate(flops=flops, bytes_accessed=1 << 16, transcendentals=0),
        name=kernel.__name__,
    )(*args)


def per_device(mass, tracer, uvel, vvel, case_east, case_north, ice_blocks):
    ncat, height, width = mass.shape
    ncomp = tracer.shape[1] + 1
    nx, ny = lax.axis_size("gx"), lax.axis_size("gy")
    local = (mass, tracer, uvel, vvel, case_east, case_north)
    pairs = (ncat * ncomp + 4) // 2
    rows = height + 2 * PAD

    edge = (ncat, ncomp, 8, width)
    pay_a, pay_b, mask = call(
        pack_rows_kernel,
        (ice_blocks,) + local,
        (shape(pairs, 8, width), shape(pairs, 8, width), shape(height, width)),
        [
            pltpu.SMEM(ice_blocks.shape, jnp.int32),
            edge,
            edge,
            (2, 8, width),
            (2, 8, width),
            pltpu.VMEM((2, 8, width), jnp.int32),
            pltpu.VMEM((2, 8, width), jnp.int32),
            pltpu.SemaphoreType.DMA((13,)),
        ],
        1 << 20,
        specs=[ANY] * 7,
    )
    both = ("gx", "gy")
    pairs_a, pairs_b = [], []
    for j in range(ny):
        for i in range(nx):
            pairs_a.append((i * ny + j, i * ny + (j ^ 1)))
            if j == ny - 1:
                pairs_b.append((i * ny + j, (nx - 1 - i) * ny + j))
            elif j:
                pairs_b.append((i * ny + j, i * ny + (j + 1 if j % 2 else j - 1)))
    got_a = lax.ppermute(pay_a, both, pairs_a)
    got_b = lax.ppermute(pay_b, both, pairs_b)

    once, twice, strips = call(
        inner_kernel,
        (mask,) + local,
        (shape(ncat, 8, rows, width), shape(ncat, 8, height, width), shape(12, rows + PAD, width)),
        [
            (4, rows, width),
            (2, 7, rows, width),
            (height, width),
            (4, 8, rows, width),
            (8, rows, width),
        ],
        1 << 27,
    )
    halo, strips, pay_w, pay_e = call(
        pack_columns_kernel,
        (got_a, got_b, strips),
        (
            shape(2 * pairs, 16, width),
            shape(12, rows + PAD, width),
            shape(2, height + 2 * DEPTH, width),
            shape(2, height + 2 * DEPTH, width),
        ),
        [(2, pairs, 8, width), (pairs, 8, width)],
        1 << 20,
        aliases={2: 1},
    )
    ahead = [(i, (i + 1) % nx) for i in range(nx)]
    back = [(target, source) for source, target in ahead]
    got_w = lax.ppermute(pay_e, "gx", ahead)
    got_e = lax.ppermute(pay_w, "gx", back)
    (rim,) = call(
        rim_kernel,
        (mask,) + local + (once, halo),
        (shape(ncat, 8, 16, width),),
        [
            (2, 4, 40, width),
            (4, 40, width),
            (2, 2, 7, 40, width),
            (2, 8, 24, width),
            (2, 8, 32, width),
            (4, 4, 8, 24, width),
            (8, 24, width),
        ],
        1 << 26,
    )
    return call(
        finish_kernel,
        (strips, got_w, got_e, twice, rim),
        (shape(ncat, height, width), shape(ncat, ncomp - 1, height, width)),
        [
            (12, rows + PAD, width),
            (4, 40, width),
            (2, 7, rows, width),
            (8, rows, width),
            (8, height, width),
            (4, 8, rows, width),
            (8, rows, width),
            (ncat, 8, height, width),
            pltpu.SemaphoreType.DMA((2, ncat)),
        ],
        1 << 26,
        out_spec=ANY,
    )


def solution(mesh):
    placed = (
        P(None, "gy", "gx"),
        P(None, None, "gy", "gx"),
        P("gy", "gx"),
        P("gy", "gx"),
        P("gy", "gx"),
        P("gy", "gx"),
        P("gy", "gx"),
    )
    return jax.shard_map(
        per_device,
        mesh=mesh,
        in_specs=placed,
        out_specs=(P(None, "gy", "gx"), P(None, None, "gy", "gx")),
        check_vma=False,
    )
```

```python
import functools

import jax
import jax.numpy as jnp
from jax import lax
from jax.experimental import pallas as pl
from jax.experimental.pallas import tpu as pltpu
from jax.sharding import PartitionSpec as P

STEPS = 2
MASS_FLOOR = 0.1
FLAGS = {}
PAD = 8
DEEP = 16
DEPTH = 2 * STEPS
STRIP = 6 * DEPTH
PER_PACK = STRIP // DEPTH
F32 = jnp.float32


def lanes_iota():
    return lax.broadcasted_iota(jnp.int32, (8, 128), 1)


def rows_iota():
    return lax.broadcasted_iota(jnp.int32, (8, 128), 0)


def roll(x, shift):
    return pltpu.roll(x, shift % 128 if isinstance(shift, int) else shift, 1)


def sel(mask, a, b):
    return jnp.where(mask, a, b)


def edge_geometry(speed, low, high, case):
    first = case == 1.0
    corner = sel(first, low, high)
    signs = sel(speed > 0.0, 1.0, -1.0)
    signed_area = sel(case == 0.0, 0.0, 0.5 * speed * corner)
    near = 0.25 * (signs - speed)
    far = 0.25 * signs - speed * (1.0 / 6.0)
    off = 0.25 - corner * (1.0 / 6.0)
    return speed, signed_area, near, far, off, sel(first, off, -off), case


def east_geometry(u, u_below, v, v_below, case):
    return edge_geometry(0.5 * (u + u_below), jnp.abs(v_below), jnp.abs(v), case)


def north_geometry(u, v, case):
    u_west, v_west = roll(u, 1), roll(v, 1)
    return edge_geometry(0.5 * (v + v_west), jnp.abs(u_west), jnp.abs(u), case)


def fill_geometry(geo, tiles, aux):
    for r in tiles:
        u, v = aux(0, r), aux(1, r)
        east = east_geometry(u, aux(0, r - 1), v, aux(1, r - 1), aux(2, r))
        north = north_geometry(u, v, aux(3, r))
        for n in range(7):
            geo[0, n, pl.ds(r, 8), :] = east[n]
            geo[1, n, pl.ds(r, 8), :] = north[n]


def ghost_aux(dst, src, base, top, height):
    for plane in range(4):
        dst[plane, pl.ds(0, 8), :] = src(plane, base)
    for r in (height - 8, height):
        at_fold = jnp.logical_and(top, rows_iota() + r >= height - 1)
        for plane in range(4):
            plain = src(plane, r)
            if plane < 2:
                ghost = -roll(src(plane, r + 1), -1)
            else:
                raw = roll(src(2, r), -1) if plane == 2 else src(3, r + 1)
                ghost = sel(raw == 0.0, 0.0, 3.0 - raw)
            dst[plane, pl.ds(r - base, 8), :] = sel(at_fold, ghost, plain)


def picks(low, high, low_slope, high_slope, forward, first):
    centre = sel(forward, low(0), high(0))
    slope = sel(forward, low_slope(0), high_slope(0))
    before = sel(forward, low(-1), high(-1))
    after = sel(forward, low(1), high(1))
    other_slope = sel(
        forward,
        sel(first, low_slope(-1), low_slope(1)),
        sel(first, high_slope(-1), high_slope(1)),
    )
    beyond = sel(forward, sel(first, low(-2), low(2)), sel(first, high(-2), high(2)))
    return centre, slope, before, after, other_slope, beyond


class Window:
    def __init__(self, load):
        self.load = load
        self.memo = {}

    def __call__(self, col, row):
        if (col, row) not in self.memo:
            self.memo[col, row] = self.load(col, row)
        return self.memo[col, row]


def picked(at, direction, masks):
    if direction == 0:
        return picks(
            lambda d: at(0, d),
            lambda d: at(1, d),
            lambda d: at(1, d) - at(-1, d),
            lambda d: at(2, d) - at(0, d),
            *masks,
        )
    return picks(
        lambda d: at(d, 0),
        lambda d: at(d, 1),
        lambda d: at(d, 1) - at(d, -1),
        lambda d: at(d, 2) - at(d, 0),
        *masks,
    )


def mass_flux(geo, at, direction):
    speed, area, near, far, off, side, case = geo
    masks = (speed > 0.0, case == 1.0)
    centre, slope, before, after, other_slope, beyond = picked(at, direction, masks)
    first = masks[1]
    other = sel(first, before, after)
    w0 = speed * (centre + near * slope)
    w1 = area * (other + far * other_slope + off * (centre - beyond))
    w2 = area * (centre + far * slope + side * (before - after))
    w1_off = w1 * off
    w2_side = w2 * side
    weights = (
        w0 - w2 + w1_off,
        w0 * near - w2 * far,
        sel(first, w1, 0.0) - w2_side,
        sel(first, 0.0, w1) + w2_side,
        w1 * far,
        w1_off,
    )
    return w0 + w1 - w2, (masks, weights)


def tracer_flux(shared, at, direction):
    masks, weights = shared
    centre, slope, before, after, other_slope, beyond = picked(at, direction, masks)
    return (
        (weights[0] * centre + weights[1] * slope)
        + (weights[2] * before + weights[3] * after)
        + (weights[4] * other_slope - weights[5] * beyond)
    )


def rotate_copies(source, low, tiles, shifted):
    for k in range(8):
        for s in [8 * t for t in range(tiles)] + [8 * tiles - 4]:
            value = source(k, low + s)
            for n, col in enumerate((1, -1, 2, -2)):
                shifted[n, k, pl.ds(s, 8), :] = roll(value, -col)


SLOT = {1: 0, -1: 1, 2: 2, -2: 3}


def window(source, shifted, low, k, row):
    def load(col, shift):
        if col == 0:
            return source(k, row + shift)
        return shifted[SLOT[col], k, pl.ds(row + shift - low, 8), :]

    return Window(load)


def load_geometry(geo, base, direction, row):
    return [geo[direction, n, pl.ds(row + base, 8), :] for n in range(7)]


def north_alone(source, shifted, low, row, data):
    at = window(source, shifted, low, 0, row)
    total, shared = mass_flux(data, at, 1)
    out = [total]
    for k in range(1, 8):
        out.append(tracer_flux(shared, window(source, shifted, low, k, row), 1))
    return out


def advance(source, geo, base, row, shifted, store, south=None):
    low = row - 2
    rotate_copies(source, low, 1, shifted)
    if south is None:
        south = load_geometry(geo, base, 1, row - 1)
    below = north_alone(source, shifted, low, row - 1, south)
    at = window(source, shifted, low, 0, row)
    east_mass, east_shared = mass_flux(load_geometry(geo, base, 0, row), at, 0)
    north_mass, north_shared = mass_flux(load_geometry(geo, base, 1, row), at, 1)
    mass = at(0, 0)
    for k in range(8):
        if k == 0:
            east, upper, carried = east_mass, north_mass, mass
        else:
            at = window(source, shifted, low, k, row)
            east = tracer_flux(east_shared, at, 0)
            upper = tracer_flux(north_shared, at, 1)
            carried = mass * at(0, 0)
        fresh = (carried - upper + below[k]) - (east - roll(east, 1))
        if k == 0:
            scale = 1.0 / jnp.maximum(fresh, MASS_FLOOR)
        else:
            fresh = fresh * scale
        store(k, row, fresh)


def advance_rows(source, geo, base, first_row, tiles, shifted, north, east, store, south=None):
    low = first_row - 2
    rotate_copies(source, low, tiles, shifted)
    below = north_alone(source, shifted, low, first_row - 1, load_geometry(geo, base, 1, first_row - 1))
    for k in range(8):
        north[k, pl.ds(8, 8), :] = below[k]

    def settle(k, offset, rotated, mass, scale, below=None):
        row = first_row + offset
        upper = north[k, pl.ds(offset + 9, 8), :]
        lower = north[k, pl.ds(offset + 8, 8), :] if below is None else below[k]
        carried = mass if k == 0 else mass * source(k, row)
        fresh = (carried - upper + lower) - (east[k] - rotated)
        if k == 0:
            scale = 1.0 / jnp.maximum(fresh, MASS_FLOOR)
        else:
            fresh = fresh * scale
        store(k, row, fresh)
        return scale

    def tile(t, carry):
        offset = 8 * t
        row = first_row + offset
        rotated = [roll(east[k], 1) for k in range(8)]
        at = window(source, shifted, low, 0, row)
        east_new, east_shared = mass_flux(load_geometry(geo, base, 0, row), at, 0)
        north_new, north_shared = mass_flux(load_geometry(geo, base, 1, row), at, 1)
        mass = source(0, row - 8)
        scale = None
        for k in range(8):
            if k:
                at = window(source, shifted, low, k, row)
                east_new = tracer_flux(east_shared, at, 0)
                north_new = tracer_flux(north_shared, at, 1)
            scale = settle(k, offset - 8, rotated[k], mass, scale)
            east[k] = east_new
            north[k, pl.ds(offset + 9, 8), :] = north_new
        return carry

    lax.fori_loop(0, tiles, tile, 0)
    offset = 8 * (tiles - 1)
    rotated = [roll(east[k], 1) for k in range(8)]
    below = None
    if south is not None:
        below = north_alone(source, shifted, low, first_row + offset - 1, south)
    mass = source(0, first_row + offset)
    scale = None
    for k in range(8):
        scale = settle(k, offset, rotated[k], mass, scale, below)


def parity():
    return lax.rem(lax.axis_index("gy"), 2)


def at_fold_block():
    return lax.axis_index("gy") == lax.axis_size("gy") - 1


def pack_rows_kernel(ice, mass, tracer, u, v, ce, cn, pay_a, pay_b, field, aux, ice_s, ints, sems):
    ncat, height, width = mass.shape
    ncomp = tracer.shape[1] + 1
    block_rows, block_cols = ice.shape
    rows = pl.ds(PAD, height)
    pairs = (
        (tracer, field.at[:, pl.ds(1, ncomp - 1), rows, :]),
        (ice, ice_s),
        (mass, field.at[:, 0, rows, :]),
        (u, aux.at[0, rows, :]),
        (v, aux.at[1, rows, :]),
        (ce, ints.at[0]),
        (cn, ints.at[1]),
    )
    copies = [pltpu.make_async_copy(src, dst, sems.at[n]) for n, (src, dst) in enumerate(pairs)]
    for copy in copies:
        copy.start()
    for copy in copies[1:]:
        copy.wait()
    lane = lanes_iota()
    for n in range(2):
        for t in range(0, height, 8):
            aux[2 + n, pl.ds(PAD + t, 8), :] = ints[n, pl.ds(t, 8), :].astype(F32)
    for b in range(block_rows):
        tile = jnp.zeros((8, width), F32)
        for n in range(block_cols):
            inside = lane >= n * (width // block_cols)
            tile = sel(inside, ice_s[b, n].astype(F32), tile)
        for t in range(0, height // block_rows, 8):
            at = pl.ds(PAD + b * (height // block_rows) + t, 8)
            for c in range(ncat):
                field[c, 0, at, :] = field[c, 0, at, :] * tile
    copies[0].wait()

    def write(dst, top):
        rows = pl.ds(PAD + (height - DEPTH if top else 0), DEPTH)
        for p in range(ncat * ncomp + 4):
            c, k = divmod(p, ncomp)
            value = field[c, k, rows, :] if c < ncat else aux[k, rows, :]
            half = (p % 2) ^ (1 if top else 0)
            dst[p // 2, pl.ds(DEPTH * half, DEPTH), :] = value

    @pl.when(parity() == 0)
    def _():
        write(pay_a, True)
        write(pay_b, False)

    @pl.when(parity() == 1)
    def _():
        write(pay_a, False)
        write(pay_b, True)


def inner_kernel(field, aux, once, twice, strips, geo, shifted, north, east):
    ncat = field.shape[0]
    height = field.shape[2] - PAD
    lane = lanes_iota()
    fill_geometry(geo, range(PAD, PAD + height, 8), lambda n, r: aux[n, pl.ds(r, 8), :])
    for plane in range(4):
        for t in range(0, height, 8):
            value = aux[plane, pl.ds(t + PAD, 8), :]
            packed = jnp.zeros((8, 128), F32)
            for c in range(ncat):
                packed = strip_place(packed, value, c * STRIP, lane)
            strips[8 + plane, pl.ds(t + DEEP, 8), :] = packed

    def category(c, carry):
        def source(k, row):
            return field[c, k, pl.ds(row + PAD, 8), :]

        def middle(k, row):
            return once[c, k, pl.ds(row + PAD, 8), :]

        def keep_once(k, row, value):
            once[c, k, pl.ds(row + PAD, 8), :] = value

        def keep_twice(k, row, value):
            twice[c, k, pl.ds(row, 8), :] = value

        for k in range(8):
            for t in range(0, height, 8):
                old = strips[k, pl.ds(t + DEEP, 8), :]
                strips[k, pl.ds(t + DEEP, 8), :] = strip_place(old, source(k, t), c * STRIP, lane)
        advance_rows(source, geo, PAD, 6, height // 8 - 1, shifted, north, east, keep_once)
        advance_rows(middle, geo, PAD, 8, height // 8 - 2, shifted, north, east, keep_twice)
        return carry

    lax.fori_loop(0, ncat, category, 0)


def strip_place(packed, value, start, lane):
    low = roll(value, start + DEPTH)
    high = roll(value, start + 5 * DEPTH)
    at = lane - start
    packed = sel(jnp.logical_and(at >= DEPTH, at < 3 * DEPTH), low, packed)
    return sel(jnp.logical_and(at >= 3 * DEPTH, at < 5 * DEPTH), high, packed)


def pack_columns_kernel(got_a, got_b, strips_in, halo, strips, pay_w, pay_e, tmp, flip):
    height = strips.shape[1] - 2 * DEEP
    lane = lanes_iota()
    even = parity() == 0
    pairs = got_a.shape[0]
    for q in range(pairs):
        tmp[0, q] = sel(even, got_b[q], got_a[q])
        tmp[1, q] = sel(even, got_a[q], got_b[q])

    @pl.when(at_fold_block())
    def _():
        for q in range(pairs):
            flip[q] = jnp.take_along_axis(tmp[1, q], 127 - lane, axis=1)
        for q in range(pairs):
            for s in range(8):
                tmp[1, q, pl.ds(s, 1), :] = flip[q, pl.ds(7 - s, 1), :]

    for p in range(2 * pairs):
        half = p % 2
        halo[p, pl.ds(PAD - DEPTH, DEPTH), :] = tmp[0, p // 2, pl.ds(DEPTH * (1 - half), DEPTH), :]
        halo[p, pl.ds(PAD, DEPTH), :] = tmp[1, p // 2, pl.ds(DEPTH * half, DEPTH), :]
    ncat = (2 * pairs - 4) // 8
    for k in range(12):
        for side in range(2):
            packed = jnp.zeros((8, 128), F32)
            for c in range(ncat):
                p = 8 * c + k if k < 8 else 8 * ncat + k - 8
                packed = strip_place(packed, halo[p, pl.ds(8 * side, 8), :], c * STRIP, lane)
            strips[k, pl.ds(DEEP - 8 + side * (height + 8), 8), :] = packed
    where = lax.rem(lane, STRIP) // DEPTH
    for g in range(2):
        for t in range(0, height + 2 * DEPTH, 8):
            west = jnp.zeros((8, 128), F32)
            east = jnp.zeros((8, 128), F32)
            for n in range(PER_PACK):
                value = strips[PER_PACK * g + n, pl.ds(t + DEEP - DEPTH, 8), :]
                west = sel(where == n, roll(value, DEPTH * (n - 1)), west)
                east = sel(where == n, roll(value, DEPTH * (n - 4)), east)
            pay_w[g, pl.ds(t, 8), :] = west
            pay_e[g, pl.ds(t, 8), :] = east


def rim_kernel(field, planes, once, halo, rim, aux, ghost, geo, edge, stage, shifted):
    ncat = field.shape[0]
    height = field.shape[2] - PAD
    own = ncat * 8
    for plane in range(4):
        aux[0, plane, pl.ds(0, 8), :] = halo[own + plane, pl.ds(0, 8), :]
        for n in range(2):
            aux[0, plane, pl.ds(8 + 8 * n, 8), :] = planes[plane, pl.ds(PAD + 8 * n, 8), :]
            aux[1, plane, pl.ds(8 * n, 8), :] = planes[plane, pl.ds(PAD + height - 16 + 8 * n, 8), :]
        aux[1, plane, pl.ds(16, 8), :] = halo[own + plane, pl.ds(8, 8), :]

    def high_aux(n, r):
        return aux[1, n, pl.ds(r - height + 16, 8), :]

    def ghost_rows(n, r):
        return ghost[n, pl.ds(r, 8), :]

    ghost_aux(ghost, high_aux, height - 16, at_fold_block(), height)
    fill_geometry(geo.at[0], (PAD - 3, PAD), lambda n, r: aux[0, n, pl.ds(r, 8), :])
    fill_geometry(geo.at[1], (1, 8), lambda n, r: aux[1, n, pl.ds(r, 8), :])
    fill_geometry(geo.at[1], (16,), ghost_rows)
    south = north_geometry(*(ghost_rows(n, 13) for n in (0, 1, 3)))

    def category(c, carry):
        for k in range(8):
            edge[0, k, pl.ds(0, 8), :] = halo[8 * c + k, pl.ds(0, 8), :]
            edge[0, k, pl.ds(8, 8), :] = field[c, k, pl.ds(PAD, 8), :]
            edge[1, k, pl.ds(0, 8), :] = field[c, k, pl.ds(PAD + height - 8, 8), :]
            edge[1, k, pl.ds(8, 8), :] = halo[8 * c + k, pl.ds(8, 8), :]
            stage[0, k, pl.ds(14, 8), :] = once[c, k, pl.ds(6 + PAD, 8), :]
            stage[1, k, pl.ds(6, 8), :] = once[c, k, pl.ds(height - 10 + PAD, 8), :]

        def low_field(k, row):
            return edge[0, k, pl.ds(row + 8, 8), :]

        def high_field(k, row):
            return edge[1, k, pl.ds(row - (height - 8), 8), :]

        def low_stage(k, row):
            return stage[0, k, pl.ds(row + 8, 8), :]

        def high_stage(k, row):
            return stage[1, k, pl.ds(row - (height - 16), 8), :]

        def keep_low(k, row, value):
            stage[0, k, pl.ds(row + 8, 8), :] = value

        def keep_high(k, row, value):
            stage[1, k, pl.ds(row - (height - 16), 8), :] = value

        def out_low(k, row, value):
            rim[c, k, pl.ds(0, 8), :] = value

        def out_high(k, row, value):
            rim[c, k, pl.ds(8, 8), :] = value

        up = 16 - height
        advance(low_field, geo.at[0], PAD, -2, shifted.at[0], keep_low)
        advance(high_field, geo.at[1], up, height - 2, shifted.at[1], keep_high, south)
        advance(low_stage, geo.at[0], PAD, 0, shifted.at[2], out_low)
        advance(high_stage, geo.at[1], up, height - 8, shifted.at[3], out_high)
        return carry

    lax.fori_loop(0, ncat, category, 0)


def finish_kernel(strips_in, got_w, got_e, twice, rim, mass_out, tracer_out, strips, ghost, geo, stage, last, shifted, north, east, whole, sems):
    ncat, height, width = mass_out.shape
    lane = lanes_iota()
    at = lax.rem(lane, STRIP)
    for k in range(12):
        g, n = divmod(k, PER_PACK)
        for t in range(0, height + 2 * DEPTH, 8):
            value = strips_in[k, pl.ds(t + DEEP - DEPTH, 8), :]
            value = sel(at < DEPTH, roll(got_w[g, pl.ds(t, 8), :], -DEPTH * n), value)
            value = sel(at >= 5 * DEPTH, roll(got_e[g, pl.ds(t, 8), :], DEPTH * (5 - n)), value)
            strips[k, pl.ds(t + DEEP - DEPTH, 8), :] = value

    def aux(n, r):
        return strips[8 + n, pl.ds(r, 8), :]

    def ghost_rows(n, r):
        return ghost[n, pl.ds(r - (height - 16 + DEEP), 8), :]

    ghost_aux(ghost, lambda n, r: aux(n, r + DEEP), height - 16, at_fold_block(), height)
    fill_geometry(geo, [DEEP - 3] + list(range(DEEP, DEEP + height, 8)), aux)
    fill_geometry(geo, (DEEP + height,), ghost_rows)
    south = north_geometry(*(ghost_rows(n, DEEP + height - 3) for n in (0, 1, 3)))

    def source(k, row):
        return strips[k, pl.ds(row + DEEP, 8), :]

    def keep(k, row, value):
        stage[k, pl.ds(row + DEEP, 8), :] = value

    def middle(k, row):
        return stage[k, pl.ds(row + DEEP, 8), :]

    def keep_last(k, row, value):
        last[k, pl.ds(row + 8, 8), :] = value

    advance_rows(source, geo, DEEP, -2, height // 8 + 1, shifted, north, east, keep, south)
    advance_rows(middle, geo, DEEP, 0, height // 8, shifted, north, east, keep_last)

    def out_copies(c):
        return (
            pltpu.make_async_copy(whole.at[c, 0], mass_out.at[c], sems.at[0, c]),
            pltpu.make_async_copy(whole.at[c, pl.ds(1, 7)], tracer_out.at[c], sems.at[1, c]),
        )

    def category(c, carry):
        for k in range(8):
            for t in range(0, height, 8):
                if t == 0:
                    value = rim[c, k, pl.ds(0, 8), :]
                elif t == height - 8:
                    value = rim[c, k, pl.ds(8, 8), :]
                else:
                    value = twice[c, k, pl.ds(t, 8), :]
                edge = last[k, pl.ds(t + 8, 8), :]
                value = sel(lane < DEPTH, roll(edge, 2 * 128 - DEPTH - c * STRIP), value)
                value = sel(lane >= 128 - DEPTH, roll(edge, 128 - 5 * DEPTH + 128 - c * STRIP), value)
                whole[c, k, pl.ds(t, 8), :] = value

        @pl.when(c > 0)
        def _():
            for copy in out_copies(c - 1):
                copy.start()

        return carry

    lax.fori_loop(0, ncat, category, 0)
    for copy in out_copies(ncat - 1):
        copy.start()
    for c in range(ncat):
        for copy in out_copies(c):
            copy.wait()


def shape(*dims):
    return jax.ShapeDtypeStruct(dims, F32)


VMEM = pl.BlockSpec(memory_space=pltpu.VMEM)
HBM = pl.BlockSpec(memory_space=pltpu.HBM)


def call(kernel, args, outs, scratch, flops, aliases=None, specs=None, out_spec=VMEM):
    return pl.pallas_call(
        kernel,
        out_shape=outs,
        in_specs=specs or [VMEM] * len(args),
        out_specs=jax.tree.map(lambda _: out_spec, outs),
        scratch_shapes=[pltpu.VMEM(dims, F32) if isinstance(dims, tuple) else dims for dims in scratch],
        input_output_aliases=aliases or {},
        compiler_params=pltpu.CompilerParams(vmem_limit_bytes=24 << 20, flags=FLAGS),
        cost_estimate=pl.CostEstimate(flops=flops, bytes_accessed=1 << 16, transcendentals=0),
        name=kernel.__name__,
    )(*args)


def per_device(mass, tracer, uvel, vvel, case_east, case_north, ice_blocks):
    ncat, height, width = mass.shape
    ncomp = tracer.shape[1] + 1
    nx, ny = lax.axis_size("gx"), lax.axis_size("gy")
    local = (mass, tracer, uvel, vvel, case_east, case_north)
    pairs = (ncat * ncomp + 4) // 2
    rows = height + 2 * PAD

    pay_a, pay_b, field, aux = call(
        pack_rows_kernel,
        (ice_blocks,) + local,
        (
            shape(pairs, 8, width),
            shape(pairs, 8, width),
            shape(ncat, ncomp, height + PAD, width),
            shape(4, height + PAD, width),
        ),
        [
            pltpu.SMEM(ice_blocks.shape, jnp.int32),
            pltpu.VMEM((2, height, width), jnp.int32),
            pltpu.SemaphoreType.DMA((7,)),
        ],
        1 << 20,
        specs=[HBM] * 7,
    )
    both = ("gx", "gy")
    pairs_a, pairs_b = [], []
    for j in range(ny):
        for i in range(nx):
            pairs_a.append((i * ny + j, i * ny + (j ^ 1)))
            if j == ny - 1:
                pairs_b.append((i * ny + j, (nx - 1 - i) * ny + j))
            elif j:
                pairs_b.append((i * ny + j, i * ny + (j + 1 if j % 2 else j - 1)))
    got_a = lax.ppermute(pay_a, both, pairs_a)
    got_b = lax.ppermute(pay_b, both, pairs_b)

    deep = height + 2 * DEEP
    once, twice, strips = call(
        inner_kernel,
        (field, aux),
        (shape(ncat, 8, rows, width), shape(ncat, 8, height, width), shape(12, deep, width)),
        [(2, 7, rows, width), (4, 8, rows, width), (8, rows, width), (8, 8, width)],
        1 << 27,
    )
    halo, strips, pay_w, pay_e = call(
        pack_columns_kernel,
        (got_a, got_b, strips),
        (
            shape(2 * pairs, 16, width),
            shape(12, deep, width),
            shape(2, height + 2 * DEPTH, width),
            shape(2, height + 2 * DEPTH, width),
        ),
        [(2, pairs, 8, width), (pairs, 8, width)],
        1 << 20,
        aliases={2: 1},
    )
    ahead = [(i, (i + 1) % nx) for i in range(nx)]
    back = [(target, source) for source, target in ahead]
    got_w = lax.ppermute(pay_e, "gx", ahead)
    got_e = lax.ppermute(pay_w, "gx", back)
    (rim,) = call(
        rim_kernel,
        (field, aux, once, halo),
        (shape(ncat, 8, 16, width),),
        [
            (2, 4, 40, width),
            (4, 40, width),
            (2, 2, 7, 40, width),
            (2, 8, 24, width),
            (2, 8, 32, width),
            (4, 4, 8, 24, width),
        ],
        1 << 26,
    )
    return call(
        finish_kernel,
        (strips, got_w, got_e, twice, rim),
        (shape(ncat, height, width), shape(ncat, ncomp - 1, height, width)),
        [
            (12, deep, width),
            (4, 40, width),
            (2, 7, deep, width),
            (8, deep, width),
            (8, height + 8, width),
            (4, 8, deep, width),
            (8, deep, width),
            (8, 8, width),
            (ncat, 8, height, width),
            pltpu.SemaphoreType.DMA((2, ncat)),
        ],
        1 << 26,
        out_spec=HBM,
    )


def solution(mesh):
    placed = (
        P(None, "gy", "gx"),
        P(None, None, "gy", "gx"),
        P("gy", "gx"),
        P("gy", "gx"),
        P("gy", "gx"),
        P("gy", "gx"),
        P("gy", "gx"),
    )
    return jax.shard_map(
        per_device,
        mesh=mesh,
        in_specs=placed,
        out_specs=(P(None, "gy", "gx"), P(None, None, "gy", "gx")),
        check_vma=False,
    )
```

```python
import functools

import jax
import jax.numpy as jnp
from jax import lax
from jax.experimental import pallas as pl
from jax.experimental.pallas import tpu as pltpu
from jax.sharding import PartitionSpec as P

STEPS = 2
MASS_FLOOR = 0.1
FLAGS = {}
PAD = 8
DEEP = 16
FRONT = 16
BACK = 24
DEPTH = 2 * STEPS
STRIP = 6 * DEPTH
PER_PACK = STRIP // DEPTH
F32 = jnp.float32


def lanes_iota():
    return lax.broadcasted_iota(jnp.int32, (8, 128), 1)


def rows_iota():
    return lax.broadcasted_iota(jnp.int32, (8, 128), 0)


def roll(x, shift):
    return pltpu.roll(x, shift % 128 if isinstance(shift, int) else shift, 1)


def sel(mask, a, b):
    return jnp.where(mask, a, b)


def edge_geometry(speed, low, high, case):
    first = case == 1.0
    corner = sel(first, low, high)
    signs = sel(speed > 0.0, 1.0, -1.0)
    signed_area = sel(case == 0.0, 0.0, 0.5 * speed * corner)
    near = 0.25 * (signs - speed)
    far = 0.25 * signs - speed * (1.0 / 6.0)
    off = 0.25 - corner * (1.0 / 6.0)
    return speed, signed_area, near, far, off, sel(first, off, -off), case


def east_geometry(u, u_below, v, v_below, case):
    return edge_geometry(0.5 * (u + u_below), jnp.abs(v_below), jnp.abs(v), case)


def north_geometry(u, v, case):
    u_west, v_west = roll(u, 1), roll(v, 1)
    return edge_geometry(0.5 * (v + v_west), jnp.abs(u_west), jnp.abs(u), case)


def fill_geometry(geo, tiles, aux):
    for r in tiles:
        u, v = aux(0, r), aux(1, r)
        east = east_geometry(u, aux(0, r - 1), v, aux(1, r - 1), aux(2, r))
        north = north_geometry(u, v, aux(3, r))
        for n in range(7):
            geo[0, n, pl.ds(r, 8), :] = east[n]
            geo[1, n, pl.ds(r, 8), :] = north[n]


def ghost_aux(dst, src, base, top, height):
    for plane in range(4):
        dst[plane, pl.ds(0, 8), :] = src(plane, base)
    for r in (height - 8, height):
        at_fold = jnp.logical_and(top, rows_iota() + r >= height - 1)
        for plane in range(4):
            plain = src(plane, r)
            if plane < 2:
                ghost = -roll(src(plane, r + 1), -1)
            else:
                raw = roll(src(2, r), -1) if plane == 2 else src(3, r + 1)
                ghost = sel(raw == 0.0, 0.0, 3.0 - raw)
            dst[plane, pl.ds(r - base, 8), :] = sel(at_fold, ghost, plain)


def picks(low, high, low_slope, high_slope, forward, first):
    centre = sel(forward, low(0), high(0))
    slope = sel(forward, low_slope(0), high_slope(0))
    before = sel(forward, low(-1), high(-1))
    after = sel(forward, low(1), high(1))
    other_slope = sel(
        forward,
        sel(first, low_slope(-1), low_slope(1)),
        sel(first, high_slope(-1), high_slope(1)),
    )
    beyond = sel(forward, sel(first, low(-2), low(2)), sel(first, high(-2), high(2)))
    return centre, slope, before, after, other_slope, beyond


class Window:
    def __init__(self, load):
        self.load = load
        self.memo = {}

    def __call__(self, col, row):
        if (col, row) not in self.memo:
            self.memo[col, row] = self.load(col, row)
        return self.memo[col, row]


def picked(at, direction, masks):
    if direction == 0:
        return picks(
            lambda d: at(0, d),
            lambda d: at(1, d),
            lambda d: at(1, d) - at(-1, d),
            lambda d: at(2, d) - at(0, d),
            *masks,
        )
    return picks(
        lambda d: at(d, 0),
        lambda d: at(d, 1),
        lambda d: at(d, 1) - at(d, -1),
        lambda d: at(d, 2) - at(d, 0),
        *masks,
    )


def mass_flux(geo, at, direction):
    speed, area, near, far, off, side, case = geo
    masks = (speed > 0.0, case == 1.0)
    centre, slope, before, after, other_slope, beyond = picked(at, direction, masks)
    first = masks[1]
    other = sel(first, before, after)
    w0 = speed * (centre + near * slope)
    w1 = area * (other + far * other_slope + off * (centre - beyond))
    w2 = area * (centre + far * slope + side * (before - after))
    w1_off = w1 * off
    w2_side = w2 * side
    weights = (
        w0 - w2 + w1_off,
        w0 * near - w2 * far,
        sel(first, w1, 0.0) - w2_side,
        sel(first, 0.0, w1) + w2_side,
        w1 * far,
        w1_off,
    )
    return w0 + w1 - w2, (masks, weights)


def tracer_flux(shared, at, direction):
    masks, weights = shared
    centre, slope, before, after, other_slope, beyond = picked(at, direction, masks)
    return (
        (weights[0] * centre + weights[1] * slope)
        + (weights[2] * before + weights[3] * after)
        + (weights[4] * other_slope - weights[5] * beyond)
    )


COLUMNS = (1, -1, 2, -2)


def rotate_copies(source, shifted, row, k):
    value = source(k, row)
    for n, col in enumerate(COLUMNS):
        shifted[k, n, pl.ds(row, 8), :] = roll(value, -col)


def window(source, shifted, k, row):
    def load(col, shift):
        if col == 0:
            return source(k, row + shift)
        return shifted[k, COLUMNS.index(col), pl.ds(row + shift, 8), :]

    return Window(load)


def north_alone(source, shifted, row, data):
    total, shared = mass_flux(data, window(source, shifted, 0, row), 1)
    out = [total]
    for k in range(1, 8):
        out.append(tracer_flux(shared, window(source, shifted, k, row), 1))
    return out


def run_tiles(count, start, stride, source, shifted, north, east, geometry, store, below=None, last_below=None, extra=None, spare=None):
    fresh_rows = (2,) if stride == 8 else (-2, 2)
    for k in range(8):
        for extra_row in (-2, 2):
            rotate_copies(source, shifted, start + extra_row, k)

    def settle(i, k, row, rotated, mass, scale, lower=None):
        upper = north[k, pl.ds(row, 8), :]
        if lower is None:
            lower = north[k, pl.ds(row - 1, 8), :] if below is None else below[1][k]
        carried = mass if k == 0 else mass * source(k, row)
        fresh = (carried - upper + lower) - (east[k] - rotated)
        if k == 0:
            scale = 1.0 / jnp.maximum(fresh, MASS_FLOOR)
        else:
            fresh = fresh * scale
        store(k, i, row, fresh)
        return scale

    def tile(i, carry):
        row = start + stride * i
        rotated = [roll(east[k], 1) for k in range(8)]
        at = window(source, shifted, 0, row)
        east_new, east_shared = mass_flux(geometry(0, i), at, 0)
        north_new, north_shared = mass_flux(geometry(1, i), at, 1)
        lower = north_alone(source, shifted, row - 1, below[0](i)) if below else None
        mass = source(0, row - stride)
        scale = None
        for k in range(8):
            if k:
                at = window(source, shifted, k, row)
                east_new = tracer_flux(east_shared, at, 0)
                north_new = tracer_flux(north_shared, at, 1)
            scale = settle(i - 1, k, row - stride, rotated[k], mass, scale)
            east[k] = east_new
            north[k, pl.ds(row, 8), :] = north_new
            if below:
                below[1][k] = lower[k]
            for fresh_row in fresh_rows:
                rotate_copies(source, shifted, row + stride + fresh_row, k)
            if extra:
                extra(i, k, row)
        return carry

    lax.fori_loop(0, count, tile, 0)
    if spare is not None:
        spare[0, pl.ds(0, 8), :] = shifted[parity(), 0, pl.ds(8, 8), :]
    row = start + stride * (count - 1)
    rotated = [roll(east[k], 1) for k in range(8)]
    lower = north_alone(source, shifted, row - 1, last_below) if last_below else [None] * 8
    mass = source(0, row)
    scale = None
    for k in range(8):
        scale = settle(count - 1, k, row, rotated[k], mass, scale, lower[k])


def parity():
    return lax.rem(lax.axis_index("gy"), 2)


def at_fold_block():
    return lax.axis_index("gy") == lax.axis_size("gy") - 1


def pack_rows_kernel(ice, mass, tracer, u, v, ce, cn, pay_a, pay_b, field, aux, ice_s, ints, sems):
    ncat, height, width = mass.shape
    ncomp = tracer.shape[1] + 1
    block_rows, block_cols = ice.shape
    rows = pl.ds(PAD, height)
    pairs = [
        (ice, ice_s),
        (u, aux.at[0, rows, :]),
        (v, aux.at[1, rows, :]),
        (ce, ints.at[0]),
        (cn, ints.at[1]),
    ]
    for c in range(ncat):
        pairs.append((mass.at[c], field.at[0, pl.ds(FRONT + c * height, height), :]))
    for c in range(ncat):
        at = pl.ds(FRONT + c * height, height)
        pairs.append((tracer.at[c], field.at[pl.ds(1, ncomp - 1), at, :]))
    copies = [pltpu.make_async_copy(src, dst, sems.at[n]) for n, (src, dst) in enumerate(pairs)]
    for copy in copies:
        copy.start()
    for copy in copies[: 5 + ncat]:
        copy.wait()
    lane = lanes_iota()
    for n in range(2):
        for t in range(0, height, 8):
            aux[2 + n, pl.ds(PAD + t, 8), :] = ints[n, pl.ds(t, 8), :].astype(F32)
    for b in range(block_rows):
        tile = jnp.zeros((8, width), F32)
        for n in range(block_cols):
            inside = lane >= n * (width // block_cols)
            tile = sel(inside, ice_s[b, n].astype(F32), tile)
        for t in range(0, height // block_rows, 8):
            for c in range(ncat):
                at = pl.ds(FRONT + c * height + b * (height // block_rows) + t, 8)
                field[0, at, :] = field[0, at, :] * tile
    for copy in copies[5 + ncat :]:
        copy.wait()

    def write(dst, top):
        first = height - DEPTH if top else 0
        for p in range(ncat * ncomp + 4):
            c, k = divmod(p, ncomp)
            if c < ncat:
                value = field[k, pl.ds(FRONT + c * height + first, DEPTH), :]
            else:
                value = aux[k, pl.ds(PAD + first, DEPTH), :]
            half = (p % 2) ^ (1 if top else 0)
            dst[p // 2, pl.ds(DEPTH * half, DEPTH), :] = value

    @pl.when(parity() == 0)
    def _():
        write(pay_a, True)
        write(pay_b, False)

    @pl.when(parity() == 1)
    def _():
        write(pay_a, False)
        write(pay_b, True)


def first_kernel(field, aux, once, strips, geo, shifted, north, east):
    height = aux.shape[1] - PAD
    ncat = (field.shape[1] - FRONT - BACK) // height
    per = height // 8
    lane = lanes_iota()
    fill_geometry(geo, range(PAD, PAD + height, 8), lambda n, r: aux[n, pl.ds(r, 8), :])
    for plane in range(4):
        for t in range(0, height, 8):
            value = aux[plane, pl.ds(t + PAD, 8), :]
            packed = jnp.zeros((8, 128), F32)
            for c in range(ncat):
                packed = strip_place(packed, value, c * STRIP, lane)
            strips[8 + plane, pl.ds(t + DEEP, 8), :] = packed

    def source(k, row):
        return field[k, pl.ds(row, 8), :]

    def geometry(direction, i):
        return [geo[direction, n, pl.ds(PAD + 8 * lax.rem(i, per), 8), :] for n in range(7)]

    def keep(k, i, row, value):
        once[k, pl.ds(row, 8), :] = value

    def place_strip(i, k, row):
        at = pl.ds(DEEP + 8 * lax.rem(i, per), 8)
        start = lax.div(i, per) * STRIP
        strips[k, at, :] = strip_place(strips[k, at, :], source(k, row), start, lane)

    run_tiles(ncat * per, FRONT, 8, source, shifted, north, east, geometry, keep, extra=place_strip, spare=once)


def strip_place(packed, value, start, lane):
    low = roll(value, start + DEPTH)
    high = roll(value, start + 5 * DEPTH)
    at = lane - start
    packed = sel(jnp.logical_and(at >= DEPTH, at < 3 * DEPTH), low, packed)
    return sel(jnp.logical_and(at >= 3 * DEPTH, at < 5 * DEPTH), high, packed)


def pack_columns_kernel(got_a, got_b, strips_in, halo, strips, pay_w, pay_e, tmp, flip):
    height = strips.shape[1] - 2 * DEEP
    lane = lanes_iota()
    even = parity() == 0
    pairs = got_a.shape[0]
    for q in range(pairs):
        tmp[0, q] = sel(even, got_b[q], got_a[q])
        tmp[1, q] = sel(even, got_a[q], got_b[q])

    @pl.when(at_fold_block())
    def _():
        for q in range(pairs):
            flip[q] = jnp.take_along_axis(tmp[1, q], 127 - lane, axis=1)
        for q in range(pairs):
            for s in range(8):
                tmp[1, q, pl.ds(s, 1), :] = flip[q, pl.ds(7 - s, 1), :]

    for p in range(2 * pairs):
        half = p % 2
        halo[p, pl.ds(PAD - DEPTH, DEPTH), :] = tmp[0, p // 2, pl.ds(DEPTH * (1 - half), DEPTH), :]
        halo[p, pl.ds(PAD, DEPTH), :] = tmp[1, p // 2, pl.ds(DEPTH * half, DEPTH), :]
    ncat = (2 * pairs - 4) // 8
    for k in range(12):
        for side in range(2):
            packed = jnp.zeros((8, 128), F32)
            for c in range(ncat):
                p = 8 * c + k if k < 8 else 8 * ncat + k - 8
                packed = strip_place(packed, halo[p, pl.ds(8 * side, 8), :], c * STRIP, lane)
            strips[k, pl.ds(DEEP - 8 + side * (height + 8), 8), :] = packed
    where = lax.rem(lane, STRIP) // DEPTH
    for g in range(2):
        for t in range(0, height + 2 * DEPTH, 8):
            west = jnp.zeros((8, 128), F32)
            east = jnp.zeros((8, 128), F32)
            for n in range(PER_PACK):
                value = strips[PER_PACK * g + n, pl.ds(t + DEEP - DEPTH, 8), :]
                west = sel(where == n, roll(value, DEPTH * (n - 1)), west)
                east = sel(where == n, roll(value, DEPTH * (n - 4)), east)
            pay_w[g, pl.ds(t, 8), :] = west
            pay_e[g, pl.ds(t, 8), :] = east


def second_kernel(field, planes, once, geo_main, halo, twice, aux, ghost, geo, south, edge, stage, shifted, north, east, held):
    height = planes.shape[1] - PAD
    ncat = (field.shape[1] - FRONT - BACK) // height
    per = height // 8
    own = ncat * 8

    def middle(k, row):
        return once[k, pl.ds(row, 8), :]

    def geometry(direction, i):
        return [geo_main[direction, n, pl.ds(PAD + 8 * lax.rem(i, per), 8), :] for n in range(7)]

    def keep(k, i, row, value):
        twice[k, pl.ds(row, 8), :] = value

    run_tiles(ncat * per, FRONT, 8, middle, shifted, north, east, geometry, keep)

    for plane in range(4):
        aux[0, plane, pl.ds(0, 8), :] = halo[own + plane, pl.ds(0, 8), :]
        for n in range(2):
            aux[0, plane, pl.ds(8 + 8 * n, 8), :] = planes[plane, pl.ds(PAD + 8 * n, 8), :]
            aux[1, plane, pl.ds(8 * n, 8), :] = planes[plane, pl.ds(PAD + height - 16 + 8 * n, 8), :]
        aux[1, plane, pl.ds(16, 8), :] = halo[own + plane, pl.ds(8, 8), :]

    def low_aux(n, r):
        return aux[0, n, pl.ds(r, 8), :]

    def high_aux(n, r):
        return aux[1, n, pl.ds(r - height + 16, 8), :]

    def ghost_rows(n, r):
        return ghost[n, pl.ds(r, 8), :]

    ghost_aux(ghost, high_aux, height - 16, at_fold_block(), height)
    fill_geometry(geo.at[0], (3, 8), low_aux)
    fill_geometry(geo.at[1], (8,), lambda n, r: aux[1, n, pl.ds(r, 8), :])
    fill_geometry(geo.at[1], (16,), ghost_rows)
    for end, (src, r) in enumerate(((low_aux, 3), (ghost_rows, 11))):
        data = north_geometry(src(0, r), src(1, r), src(3, r))
        for n in range(7):
            south[end, n] = data[n]
    for c in range(ncat):
        base = FRONT + c * height
        at = FRONT + 32 * c
        for k in range(8):
            edge[k, pl.ds(at, 8), :] = halo[8 * c + k, pl.ds(0, 8), :]
            edge[k, pl.ds(at + 8, 8), :] = field[k, pl.ds(base, 8), :]
            edge[k, pl.ds(at + 16, 8), :] = field[k, pl.ds(base + height - 8, 8), :]
            edge[k, pl.ds(at + 24, 8), :] = halo[8 * c + k, pl.ds(8, 8), :]
            stage[k, pl.ds(at + 12, 8), :] = once[k, pl.ds(base + 4, 8), :]
            stage[k, pl.ds(at + 16, 8), :] = once[k, pl.ds(base + height - 14, 8), :]
            stage[k, pl.ds(at + 18, 8), :] = once[k, pl.ds(base + height - 12, 8), :]

    def end_of(i):
        return lax.rem(i + 2, 2)

    def edge_source(k, row):
        return edge[k, pl.ds(row, 8), :]

    def stage_source(k, row):
        return stage[k, pl.ds(row, 8), :]

    def edge_geometry_at(direction, i):
        end = end_of(i)
        return [geo[end, direction, n, pl.ds(4 + 8 * end, 8), :] for n in range(7)]

    def stage_geometry_at(direction, i):
        end = end_of(i)
        return [geo[end, direction, n, pl.ds(7 + 2 * end, 8), :] for n in range(7)]

    def south_at(i):
        end = end_of(i)
        return [south[end, n] for n in range(7)]

    def keep_stage(k, i, row, value):
        stage[k, pl.ds(row + 6 * end_of(i), 8), :] = value

    inside = jnp.logical_and(rows_iota() >= 1, rows_iota() <= 6)

    def keep_rim(k, i, row, value):
        c = lax.div(i + 2, 2) - 1
        at = pl.ds(FRONT + height * c - 1 + (height - 6) * end_of(i), 8)
        twice[k, at, :] = sel(inside, value, twice[k, at, :])

    run_tiles(
        2 * ncat, FRONT + 4, 16, edge_source, shifted, north, east, edge_geometry_at, keep_stage, below=(south_at, held)
    )
    run_tiles(2 * ncat, FRONT + 7, 16, stage_source, shifted, north, east, stage_geometry_at, keep_rim, spare=twice)


def finish_kernel(strips_in, got_w, got_e, twice, mass_out, tracer_out, strips, ghost, geo, stage, last, shifted, north, east, whole, sems):
    ncat, height, width = mass_out.shape
    lane = lanes_iota()
    at = lax.rem(lane, STRIP)
    for k in range(12):
        g, n = divmod(k, PER_PACK)
        for t in range(0, height + 2 * DEPTH, 8):
            value = strips_in[k, pl.ds(t + DEEP - DEPTH, 8), :]
            value = sel(at < DEPTH, roll(got_w[g, pl.ds(t, 8), :], -DEPTH * n), value)
            value = sel(at >= 5 * DEPTH, roll(got_e[g, pl.ds(t, 8), :], DEPTH * (5 - n)), value)
            strips[k, pl.ds(t + DEEP - DEPTH, 8), :] = value

    def aux(n, r):
        return strips[8 + n, pl.ds(r, 8), :]

    def ghost_rows(n, r):
        return ghost[n, pl.ds(r - (height - 16 + DEEP), 8), :]

    ghost_aux(ghost, lambda n, r: aux(n, r + DEEP), height - 16, at_fold_block(), height)
    fill_geometry(geo, [DEEP - 4] + list(range(DEEP, DEEP + height, 8)), aux)
    fill_geometry(geo, (DEEP + height,), ghost_rows)
    south = north_geometry(*(ghost_rows(n, DEEP + height - 5) for n in (0, 1, 3)))

    def source(k, row):
        return strips[k, pl.ds(row, 8), :]

    def middle(k, row):
        return stage[k, pl.ds(row, 8), :]

    def keep(k, i, row, value):
        stage[k, pl.ds(row, 8), :] = value

    def keep_last(k, i, row, value):
        last[k, pl.ds(row, 8), :] = value

    def geometry(direction, i):
        return [geo[direction, n, pl.ds(DEEP - 4 + 8 * i, 8), :] for n in range(7)]

    count = height // 8 + 1
    run_tiles(count, DEEP - 4, 8, source, shifted, north, east, geometry, keep, last_below=south)
    run_tiles(count, DEEP - 4, 8, middle, shifted, north, east, geometry, keep_last)

    def out_copies(c):
        return (
            pltpu.make_async_copy(whole.at[c, 0], mass_out.at[c], sems.at[0, c]),
            pltpu.make_async_copy(whole.at[c, pl.ds(1, 7)], tracer_out.at[c], sems.at[1, c]),
        )

    def category(c, carry):
        for k in range(8):
            for t in range(0, height, 8):
                value = twice[k, pl.ds(FRONT + c * height + t, 8), :]
                edge = last[k, pl.ds(t + DEEP, 8), :]
                value = sel(lane < DEPTH, roll(edge, 2 * 128 - DEPTH - c * STRIP), value)
                value = sel(lane >= 128 - DEPTH, roll(edge, 128 - 5 * DEPTH + 128 - c * STRIP), value)
                whole[c, k, pl.ds(t, 8), :] = value

        @pl.when(c > 0)
        def _():
            for copy in out_copies(c - 1):
                copy.start()

        return carry

    lax.fori_loop(0, ncat, category, 0)
    for copy in out_copies(ncat - 1):
        copy.start()
    for c in range(ncat):
        for copy in out_copies(c):
            copy.wait()


def shape(*dims):
    return jax.ShapeDtypeStruct(dims, F32)


VMEM = pl.BlockSpec(memory_space=pltpu.VMEM)
HBM = pl.BlockSpec(memory_space=pltpu.HBM)


def call(kernel, args, outs, scratch, flops, aliases=None, specs=None, out_spec=VMEM):
    return pl.pallas_call(
        kernel,
        out_shape=outs,
        in_specs=specs or [VMEM] * len(args),
        out_specs=jax.tree.map(lambda _: out_spec, outs),
        scratch_shapes=[pltpu.VMEM(dims, F32) if isinstance(dims, tuple) else dims for dims in scratch],
        input_output_aliases=aliases or {},
        compiler_params=pltpu.CompilerParams(vmem_limit_bytes=24 << 20, flags=FLAGS),
        cost_estimate=pl.CostEstimate(flops=flops, bytes_accessed=1 << 16, transcendentals=0),
        name=kernel.__name__,
    )(*args)


def per_device(mass, tracer, uvel, vvel, case_east, case_north, ice_blocks):
    ncat, height, width = mass.shape
    ncomp = tracer.shape[1] + 1
    nx, ny = lax.axis_size("gx"), lax.axis_size("gy")
    local = (mass, tracer, uvel, vvel, case_east, case_north)
    pairs = (ncat * ncomp + 4) // 2
    rows = height + 2 * PAD
    tall = FRONT + ncat * height + BACK
    block = FRONT + 32 * ncat + BACK
    deep = height + 2 * DEEP

    pay_a, pay_b, field, aux = call(
        pack_rows_kernel,
        tuple(pltpu.with_memory_space_constraint(x, pltpu.HBM) for x in (ice_blocks,) + local),
        (
            shape(pairs, 8, width),
            shape(pairs, 8, width),
            shape(ncomp, tall, width),
            shape(4, height + PAD, width),
        ),
        [
            pltpu.SMEM(ice_blocks.shape, jnp.int32),
            pltpu.VMEM((2, height, width), jnp.int32),
            pltpu.SemaphoreType.DMA((5 + 2 * ncat,)),
        ],
        1 << 20,
        specs=[HBM] * 7,
    )
    both = ("gx", "gy")
    pairs_a, pairs_b = [], []
    for j in range(ny):
        for i in range(nx):
            pairs_a.append((i * ny + j, i * ny + (j ^ 1)))
            if j == ny - 1:
                pairs_b.append((i * ny + j, (nx - 1 - i) * ny + j))
            elif j:
                pairs_b.append((i * ny + j, i * ny + (j + 1 if j % 2 else j - 1)))
    got_a = lax.ppermute(pay_a, both, pairs_a)
    got_b = lax.ppermute(pay_b, both, pairs_b)

    once, strips, geo = call(
        first_kernel,
        (field, aux),
        (shape(8, tall, width), shape(12, deep, width), shape(2, 7, rows, width)),
        [(8, 4, tall, width), (8, tall, width), (8, 8, width)],
        1 << 27,
    )
    halo, strips, pay_w, pay_e = call(
        pack_columns_kernel,
        (got_a, got_b, strips),
        (
            shape(2 * pairs, 16, width),
            shape(12, deep, width),
            shape(2, height + 2 * DEPTH, width),
            shape(2, height + 2 * DEPTH, width),
        ),
        [(2, pairs, 8, width), (pairs, 8, width)],
        1 << 20,
        aliases={2: 1},
    )
    ahead = [(i, (i + 1) % nx) for i in range(nx)]
    back = [(target, source) for source, target in ahead]
    got_w = lax.ppermute(pay_e, "gx", ahead)
    got_e = lax.ppermute(pay_w, "gx", back)
    (twice,) = call(
        second_kernel,
        (field, aux, once, geo, halo),
        (shape(8, tall, width),),
        [
            (2, 4, 40, width),
            (4, 40, width),
            (2, 2, 7, 40, width),
            (2, 7, 8, width),
            (8, block, width),
            (8, block, width),
            (8, 4, tall, width),
            (8, tall, width),
            (8, 8, width),
            (8, 8, width),
        ],
        1 << 27,
    )
    return call(
        finish_kernel,
        (strips, got_w, got_e, twice),
        (shape(ncat, height, width), shape(ncat, ncomp - 1, height, width)),
        [
            (12, deep, width),
            (4, 40, width),
            (2, 7, deep, width),
            (8, deep, width),
            (8, deep, width),
            (8, 4, deep, width),
            (8, deep, width),
            (8, 8, width),
            (ncat, 8, height, width),
            pltpu.SemaphoreType.DMA((2, ncat)),
        ],
        1 << 26,
        out_spec=HBM,
    )


def solution(mesh):
    placed = (
        P(None, "gy", "gx"),
        P(None, None, "gy", "gx"),
        P("gy", "gx"),
        P("gy", "gx"),
        P("gy", "gx"),
        P("gy", "gx"),
        P("gy", "gx"),
    )
    return jax.shard_map(
        per_device,
        mesh=mesh,
        in_specs=placed,
        out_specs=(P(None, "gy", "gx"), P(None, None, "gy", "gx")),
        check_vma=False,
    )
```

```python
import functools

import jax
import jax.numpy as jnp
from jax import lax
from jax.experimental import pallas as pl
from jax.experimental.pallas import tpu as pltpu
from jax.sharding import PartitionSpec as P

STEPS = 2
MASS_FLOOR = 0.1
FLAGS = {}
PAD = 8
DEEP = 16
FRONT = 16
BACK = 72
DEPTH = 2 * STEPS
STRIP = 6 * DEPTH
PER_PACK = STRIP // DEPTH
F32 = jnp.float32


def lanes_iota():
    return lax.broadcasted_iota(jnp.int32, (8, 128), 1)


def rows_iota():
    return lax.broadcasted_iota(jnp.int32, (8, 128), 0)


def roll(x, shift):
    return pltpu.roll(x, shift % 128 if isinstance(shift, int) else shift, 1)


def sel(mask, a, b):
    return jnp.where(mask, a, b)


def edge_geometry(speed, low, high, case):
    first = case == 1.0
    corner = sel(first, low, high)
    signs = sel(speed > 0.0, 1.0, -1.0)
    signed_area = sel(case == 0.0, 0.0, 0.5 * speed * corner)
    near = 0.25 * (signs - speed)
    far = 0.25 * signs - speed * (1.0 / 6.0)
    off = 0.25 - corner * (1.0 / 6.0)
    return speed, signed_area, near, far, off, sel(first, off, -off), case


def east_geometry(u, u_below, v, v_below, case):
    return edge_geometry(0.5 * (u + u_below), jnp.abs(v_below), jnp.abs(v), case)


def north_geometry(u, v, case):
    u_west, v_west = roll(u, 1), roll(v, 1)
    return edge_geometry(0.5 * (v + v_west), jnp.abs(u_west), jnp.abs(u), case)


def fill_geometry(geo, tiles, aux):
    for r in tiles:
        u, v = aux(0, r), aux(1, r)
        east = east_geometry(u, aux(0, r - 1), v, aux(1, r - 1), aux(2, r))
        north = north_geometry(u, v, aux(3, r))
        for n in range(7):
            geo[0, n, pl.ds(r, 8), :] = east[n]
            geo[1, n, pl.ds(r, 8), :] = north[n]


def ghost_aux(dst, src, base, top, height):
    for plane in range(4):
        dst[plane, pl.ds(0, 8), :] = src(plane, base)
    for r in (height - 8, height):
        at_fold = jnp.logical_and(top, rows_iota() + r >= height - 1)
        for plane in range(4):
            plain = src(plane, r)
            if plane < 2:
                ghost = -roll(src(plane, r + 1), -1)
            else:
                raw = roll(src(2, r), -1) if plane == 2 else src(3, r + 1)
                ghost = sel(raw == 0.0, 0.0, 3.0 - raw)
            dst[plane, pl.ds(r - base, 8), :] = sel(at_fold, ghost, plain)


def picks(low, high, low_slope, high_slope, forward, first):
    centre = sel(forward, low(0), high(0))
    slope = sel(forward, low_slope(0), high_slope(0))
    before = sel(forward, low(-1), high(-1))
    after = sel(forward, low(1), high(1))
    other_slope = sel(
        forward,
        sel(first, low_slope(-1), low_slope(1)),
        sel(first, high_slope(-1), high_slope(1)),
    )
    beyond = sel(forward, sel(first, low(-2), low(2)), sel(first, high(-2), high(2)))
    return centre, slope, before, after, other_slope, beyond


class Window:
    def __init__(self, load):
        self.load = load
        self.memo = {}

    def __call__(self, col, row):
        if (col, row) not in self.memo:
            self.memo[col, row] = self.load(col, row)
        return self.memo[col, row]


def picked(at, direction, masks):
    if direction == 0:
        return picks(
            lambda d: at(0, d),
            lambda d: at(1, d),
            lambda d: at(1, d) - at(-1, d),
            lambda d: at(2, d) - at(0, d),
            *masks,
        )
    return picks(
        lambda d: at(d, 0),
        lambda d: at(d, 1),
        lambda d: at(d, 1) - at(d, -1),
        lambda d: at(d, 2) - at(d, 0),
        *masks,
    )


def mass_flux(geo, at, direction):
    speed, area, near, far, off, side, case = geo
    masks = (speed > 0.0, case == 1.0)
    centre, slope, before, after, other_slope, beyond = picked(at, direction, masks)
    first = masks[1]
    other = sel(first, before, after)
    w0 = speed * (centre + near * slope)
    w1 = area * (other + far * other_slope + off * (centre - beyond))
    w2 = area * (centre + far * slope + side * (before - after))
    w1_off = w1 * off
    w2_side = w2 * side
    weights = (
        w0 - w2 + w1_off,
        w0 * near - w2 * far,
        sel(first, w1, 0.0) - w2_side,
        sel(first, 0.0, w1) + w2_side,
        w1 * far,
        w1_off,
    )
    return w0 + w1 - w2, (masks, weights)


def tracer_flux(shared, at, direction):
    masks, weights = shared
    centre, slope, before, after, other_slope, beyond = picked(at, direction, masks)
    return (
        (weights[0] * centre + weights[1] * slope)
        + (weights[2] * before + weights[3] * after)
        + (weights[4] * other_slope - weights[5] * beyond)
    )


COLUMNS = (1, -1, 2, -2)


def rotate_copies(source, shifted, row, k):
    value = source(k, row)
    for n, col in enumerate(COLUMNS):
        shifted[k, n, pl.ds(row, 8), :] = roll(value, -col)


def window(source, shifted, k, row):
    def load(col, shift):
        if col == 0:
            return source(k, row + shift)
        return shifted[k, COLUMNS.index(col), pl.ds(row + shift, 8), :]

    return Window(load)


def north_alone(source, shifted, row, data):
    total, shared = mass_flux(data, window(source, shifted, 0, row), 1)
    out = [total]
    for k in range(1, 8):
        out.append(tracer_flux(shared, window(source, shifted, k, row), 1))
    return out


def run_tiles(count, start, stride, source, shifted, north, east, geometry, store, below=None, last_below=None, extra=None, spare=None, group=2):
    fresh_rows = (2,) if stride == 8 else (-2, 2)
    first_rows = {stride * j + r for j in range(group) for r in fresh_rows} | {-2, 2}
    for k in range(8):
        for r in sorted(first_rows):
            rotate_copies(source, shifted, start + r, k)

    def settle(i, k, row, rotated, mass, scale, lower=None):
        upper = north[k, pl.ds(row, 8), :]
        if lower is None:
            lower = north[k, pl.ds(row - 1, 8), :] if below is None else below[1][k]
        carried = mass if k == 0 else mass * source(k, row)
        fresh = (carried - upper + lower) - (east[k] - rotated)
        if k == 0:
            scale = 1.0 / jnp.maximum(fresh, MASS_FLOOR)
        else:
            fresh = fresh * scale
        store(k, i, row, fresh)
        return scale

    def tile(i):
        row = start + stride * i
        rotated = [roll(east[k], 1) for k in range(8)]
        copies = []
        for k in range(8):
            for fresh_row in fresh_rows:
                ahead = row + stride * group + fresh_row
                value = source(k, ahead)
                copies.append((k, ahead, [roll(value, -col) for col in COLUMNS]))
        later = [extra(i, k, row) for k in range(8)] if extra else []
        at = window(source, shifted, 0, row)
        east_new, east_shared = mass_flux(geometry(0, i), at, 0)
        north_new, north_shared = mass_flux(geometry(1, i), at, 1)
        lower = north_alone(source, shifted, row - 1, below[0](i)) if below else None
        mass = source(0, row - stride)
        scale = None
        for k in range(8):
            if k:
                at = window(source, shifted, k, row)
                east_new = tracer_flux(east_shared, at, 0)
                north_new = tracer_flux(north_shared, at, 1)
            scale = settle(i - 1, k, row - stride, rotated[k], mass, scale)
            east[k] = east_new
            north[k, pl.ds(row, 8), :] = north_new
            if below:
                below[1][k] = lower[k]
        for k, ahead, moved in copies:
            for n in range(4):
                shifted[k, n, pl.ds(ahead, 8), :] = moved[n]
        for finish in later:
            finish()

    def tiles(n, carry):
        for j in range(group):
            tile(n * group + j)
        return carry

    lax.fori_loop(0, count // group, tiles, 0)
    if spare is not None:
        spare[0, pl.ds(0, 8), :] = shifted[parity(), 0, pl.ds(8, 8), :]
    row = start + stride * (count - 1)
    rotated = [roll(east[k], 1) for k in range(8)]
    lower = north_alone(source, shifted, row - 1, last_below) if last_below else [None] * 8
    mass = source(0, row)
    scale = None
    for k in range(8):
        scale = settle(count - 1, k, row, rotated[k], mass, scale, lower[k])


def parity():
    return lax.rem(lax.axis_index("gy"), 2)


def at_fold_block():
    return lax.axis_index("gy") == lax.axis_size("gy") - 1


def pack_rows_kernel(ice, mass, tracer, u, v, ce, cn, pay_a, pay_b, field, aux, ice_s, ints, sems):
    ncat, height, width = mass.shape
    ncomp = tracer.shape[1] + 1
    block_rows, block_cols = ice.shape
    rows = pl.ds(PAD, height)
    pairs = [
        (ice, ice_s),
        (u, aux.at[0, rows, :]),
        (v, aux.at[1, rows, :]),
        (ce, ints.at[0]),
        (cn, ints.at[1]),
    ]
    for c in range(ncat):
        pairs.append((mass.at[c], field.at[0, pl.ds(FRONT + c * height, height), :]))
    for c in range(ncat):
        at = pl.ds(FRONT + c * height, height)
        pairs.append((tracer.at[c], field.at[pl.ds(1, ncomp - 1), at, :]))
    copies = [pltpu.make_async_copy(src, dst, sems.at[n]) for n, (src, dst) in enumerate(pairs)]
    for copy in copies:
        copy.start()
    for copy in copies[: 5 + ncat]:
        copy.wait()
    lane = lanes_iota()
    for n in range(2):
        for t in range(0, height, 8):
            aux[2 + n, pl.ds(PAD + t, 8), :] = ints[n, pl.ds(t, 8), :].astype(F32)
    for b in range(block_rows):
        tile = jnp.zeros((8, width), F32)
        for n in range(block_cols):
            inside = lane >= n * (width // block_cols)
            tile = sel(inside, ice_s[b, n].astype(F32), tile)
        for t in range(0, height // block_rows, 8):
            for c in range(ncat):
                at = pl.ds(FRONT + c * height + b * (height // block_rows) + t, 8)
                field[0, at, :] = field[0, at, :] * tile
    for copy in copies[5 + ncat :]:
        copy.wait()

    def write(dst, top):
        first = height - DEPTH if top else 0
        for p in range(ncat * ncomp + 4):
            c, k = divmod(p, ncomp)
            if c < ncat:
                value = field[k, pl.ds(FRONT + c * height + first, DEPTH), :]
            else:
                value = aux[k, pl.ds(PAD + first, DEPTH), :]
            half = (p % 2) ^ (1 if top else 0)
            dst[p // 2, pl.ds(DEPTH * half, DEPTH), :] = value

    @pl.when(parity() == 0)
    def _():
        write(pay_a, True)
        write(pay_b, False)

    @pl.when(parity() == 1)
    def _():
        write(pay_a, False)
        write(pay_b, True)


def first_kernel(field, aux, once, strips, geo, shifted, north, east):
    height = aux.shape[1] - PAD
    ncat = (field.shape[1] - FRONT - BACK) // height
    per = height // 8
    lane = lanes_iota()
    fill_geometry(geo, range(PAD, PAD + height, 8), lambda n, r: aux[n, pl.ds(r, 8), :])
    where = strip_index(lane)
    for plane in range(4):
        for t in range(0, height, 8):
            strips[8 + plane, pl.ds(t + DEEP, 8), :] = gather(aux[plane, pl.ds(t + PAD, 8), :], where)

    def source(k, row):
        return field[k, pl.ds(row, 8), :]

    def geometry(direction, i):
        return [geo[direction, n, pl.ds(PAD + 8 * lax.rem(i, per), 8), :] for n in range(7)]

    def keep(k, i, row, value):
        once[k, pl.ds(row, 8), :] = value

    def place_strip(i, k, row):
        at = pl.ds(DEEP + 8 * lax.rem(i, per), 8)
        start = lax.div(i, per) * STRIP
        moved = gather(source(k, row), where)

        def finish():
            strips[k, at, :] = strip_merge(strips[k, at, :], moved, start, lane)

        return finish

    run_tiles(ncat * per, FRONT, 8, source, shifted, north, east, geometry, keep, extra=place_strip, spare=once, group=5)


def gather(value, index):
    return jnp.take_along_axis(value, index, axis=1, mode="promise_in_bounds")


def strip_index(lane):
    at = lax.rem(lane, STRIP)
    index = sel(at < 3 * DEPTH, at - DEPTH, at + 128 - 5 * DEPTH)
    return jnp.clip(index, 0, 127)


def strip_merge(packed, moved, start, lane):
    at = lane - start
    return sel(jnp.logical_and(at >= DEPTH, at < 5 * DEPTH), moved, packed)


def pack_columns_kernel(got_a, got_b, strips_in, halo, strips, pay_w, pay_e, tmp, flip):
    height = strips.shape[1] - 3 * DEEP
    lane = lanes_iota()
    even = parity() == 0
    pairs = got_a.shape[0]
    for q in range(pairs):
        tmp[0, q] = sel(even, got_b[q], got_a[q])
        tmp[1, q] = sel(even, got_a[q], got_b[q])

    @pl.when(at_fold_block())
    def _():
        for q in range(pairs):
            flip[q] = gather(tmp[1, q], 127 - lane)
        for q in range(pairs):
            for s in range(8):
                tmp[1, q, pl.ds(s, 1), :] = flip[q, pl.ds(7 - s, 1), :]

    for p in range(2 * pairs):
        half = p % 2
        halo[p, pl.ds(PAD - DEPTH, DEPTH), :] = tmp[0, p // 2, pl.ds(DEPTH * (1 - half), DEPTH), :]
        halo[p, pl.ds(PAD, DEPTH), :] = tmp[1, p // 2, pl.ds(DEPTH * half, DEPTH), :]
    ncat = (2 * pairs - 4) // 8
    index = strip_index(lane)
    for k in range(12):
        for side in range(2):
            at = pl.ds(8 * side, 8)
            if k < 8:
                packed = jnp.zeros((8, 128), F32)
                for c in range(ncat):
                    packed = strip_merge(packed, gather(halo[8 * c + k, at, :], index), c * STRIP, lane)
            else:
                packed = gather(halo[8 * ncat + k - 8, at, :], index)
            strips[k, pl.ds(DEEP - 8 + side * (height + 8), 8), :] = packed
    where = lax.rem(lane, STRIP) // DEPTH
    for g in range(2):
        for t in range(0, height + 2 * DEPTH, 8):
            west = jnp.zeros((8, 128), F32)
            east = jnp.zeros((8, 128), F32)
            for n in range(PER_PACK):
                value = strips[PER_PACK * g + n, pl.ds(t + DEEP - DEPTH, 8), :]
                west = sel(where == n, roll(value, DEPTH * (n - 1)), west)
                east = sel(where == n, roll(value, DEPTH * (n - 4)), east)
            pay_w[g, pl.ds(t, 8), :] = west
            pay_e[g, pl.ds(t, 8), :] = east


def second_kernel(field, planes, once, geo_main, halo, twice, aux, ghost, geo, south, edge, stage, shifted, north, east, held):
    height = planes.shape[1] - PAD
    ncat = (field.shape[1] - FRONT - BACK) // height
    per = height // 8
    own = ncat * 8

    def middle(k, row):
        return once[k, pl.ds(row, 8), :]

    def geometry(direction, i):
        return [geo_main[direction, n, pl.ds(PAD + 8 * lax.rem(i, per), 8), :] for n in range(7)]

    def keep(k, i, row, value):
        twice[k, pl.ds(row, 8), :] = value

    run_tiles(ncat * per, FRONT, 8, middle, shifted, north, east, geometry, keep, group=5)

    for plane in range(4):
        aux[0, plane, pl.ds(0, 8), :] = halo[own + plane, pl.ds(0, 8), :]
        for n in range(2):
            aux[0, plane, pl.ds(8 + 8 * n, 8), :] = planes[plane, pl.ds(PAD + 8 * n, 8), :]
            aux[1, plane, pl.ds(8 * n, 8), :] = planes[plane, pl.ds(PAD + height - 16 + 8 * n, 8), :]
        aux[1, plane, pl.ds(16, 8), :] = halo[own + plane, pl.ds(8, 8), :]

    def low_aux(n, r):
        return aux[0, n, pl.ds(r, 8), :]

    def high_aux(n, r):
        return aux[1, n, pl.ds(r - height + 16, 8), :]

    def ghost_rows(n, r):
        return ghost[n, pl.ds(r, 8), :]

    ghost_aux(ghost, high_aux, height - 16, at_fold_block(), height)
    fill_geometry(geo.at[0], (3, 8), low_aux)
    fill_geometry(geo.at[1], (8,), lambda n, r: aux[1, n, pl.ds(r, 8), :])
    fill_geometry(geo.at[1], (16,), ghost_rows)
    for end, (src, r) in enumerate(((low_aux, 3), (ghost_rows, 11))):
        data = north_geometry(src(0, r), src(1, r), src(3, r))
        for n in range(7):
            south[end, n] = data[n]
    for c in range(ncat):
        base = FRONT + c * height
        at = FRONT + 32 * c
        for k in range(8):
            edge[k, pl.ds(at, 8), :] = halo[8 * c + k, pl.ds(0, 8), :]
            edge[k, pl.ds(at + 8, 8), :] = field[k, pl.ds(base, 8), :]
            edge[k, pl.ds(at + 16, 8), :] = field[k, pl.ds(base + height - 8, 8), :]
            edge[k, pl.ds(at + 24, 8), :] = halo[8 * c + k, pl.ds(8, 8), :]
            stage[k, pl.ds(at + 12, 8), :] = once[k, pl.ds(base + 4, 8), :]
            stage[k, pl.ds(at + 16, 8), :] = once[k, pl.ds(base + height - 14, 8), :]
            stage[k, pl.ds(at + 18, 8), :] = once[k, pl.ds(base + height - 12, 8), :]

    def end_of(i):
        return lax.rem(i + 2, 2)

    def edge_source(k, row):
        return edge[k, pl.ds(row, 8), :]

    def stage_source(k, row):
        return stage[k, pl.ds(row, 8), :]

    def edge_geometry_at(direction, i):
        end = end_of(i)
        return [geo[end, direction, n, pl.ds(4 + 8 * end, 8), :] for n in range(7)]

    def stage_geometry_at(direction, i):
        end = end_of(i)
        return [geo[end, direction, n, pl.ds(7 + 2 * end, 8), :] for n in range(7)]

    def south_at(i):
        end = end_of(i)
        return [south[end, n] for n in range(7)]

    def keep_stage(k, i, row, value):
        stage[k, pl.ds(row + 6 * end_of(i), 8), :] = value

    inside = jnp.logical_and(rows_iota() >= 1, rows_iota() <= 6)

    def keep_rim(k, i, row, value):
        c = lax.div(i + 2, 2) - 1
        at = pl.ds(FRONT + height * c - 1 + (height - 6) * end_of(i), 8)
        twice[k, at, :] = sel(inside, value, twice[k, at, :])

    run_tiles(
        2 * ncat, FRONT + 4, 16, edge_source, shifted, north, east, edge_geometry_at, keep_stage, below=(south_at, held)
    )
    run_tiles(2 * ncat, FRONT + 7, 16, stage_source, shifted, north, east, stage_geometry_at, keep_rim, spare=twice)


def finish_kernel(strips_in, got_w, got_e, twice, mass_out, tracer_out, strips, ghost, geo, stage, last, shifted, north, east, whole, sems):
    ncat, height, width = mass_out.shape
    lane = lanes_iota()
    at = lax.rem(lane, STRIP)
    for k in range(12):
        g, n = divmod(k, PER_PACK)
        for t in range(0, height + 2 * DEPTH, 8):
            value = strips_in[k, pl.ds(t + DEEP - DEPTH, 8), :]
            value = sel(at < DEPTH, roll(got_w[g, pl.ds(t, 8), :], -DEPTH * n), value)
            value = sel(at >= 5 * DEPTH, roll(got_e[g, pl.ds(t, 8), :], DEPTH * (5 - n)), value)
            strips[k, pl.ds(t + DEEP - DEPTH, 8), :] = value

    def aux(n, r):
        return strips[8 + n, pl.ds(r, 8), :]

    def ghost_rows(n, r):
        return ghost[n, pl.ds(r - (height - 16 + DEEP), 8), :]

    ghost_aux(ghost, lambda n, r: aux(n, r + DEEP), height - 16, at_fold_block(), height)
    fill_geometry(geo, [DEEP - 4] + list(range(DEEP, DEEP + height, 8)), aux)
    fill_geometry(geo, (DEEP + height,), ghost_rows)
    south = north_geometry(*(ghost_rows(n, DEEP + height - 5) for n in (0, 1, 3)))

    def source(k, row):
        return strips[k, pl.ds(row, 8), :]

    def middle(k, row):
        return stage[k, pl.ds(row, 8), :]

    def keep(k, i, row, value):
        stage[k, pl.ds(row, 8), :] = value

    def keep_last(k, i, row, value):
        last[k, pl.ds(row, 8), :] = value

    def geometry(direction, i):
        return [geo[direction, n, pl.ds(DEEP - 4 + 8 * i, 8), :] for n in range(7)]

    count = height // 8 + 1
    run_tiles(count, DEEP - 4, 8, source, shifted, north, east, geometry, keep, last_below=south, group=3)
    run_tiles(count, DEEP - 4, 8, middle, shifted, north, east, geometry, keep_last, group=3)

    def out_copies(c):
        return (
            pltpu.make_async_copy(whole.at[c, 0], mass_out.at[c], sems.at[0, c]),
            pltpu.make_async_copy(whole.at[c, pl.ds(1, 7)], tracer_out.at[c], sems.at[1, c]),
        )

    edges = jnp.logical_or(lane < DEPTH, lane >= 128 - DEPTH)
    for c in range(ncat):
        index = sel(lane < 64, lane + DEPTH, lane - 128 + 5 * DEPTH) + c * STRIP
        index = jnp.clip(index, 0, 127)
        for k in range(8):
            for t in range(0, height, 8):
                value = twice[k, pl.ds(FRONT + c * height + t, 8), :]
                moved = gather(last[k, pl.ds(t + DEEP, 8), :], index)
                whole[c, k, pl.ds(t, 8), :] = sel(edges, moved, value)
        if c:
            for copy in out_copies(c - 1):
                copy.start()
    for copy in out_copies(ncat - 1):
        copy.start()
    for c in range(ncat):
        for copy in out_copies(c):
            copy.wait()


def shape(*dims):
    return jax.ShapeDtypeStruct(dims, F32)


VMEM = pl.BlockSpec(memory_space=pltpu.VMEM)
HBM = pl.BlockSpec(memory_space=pltpu.HBM)


def call(kernel, args, outs, scratch, flops, aliases=None, specs=None, out_spec=VMEM):
    return pl.pallas_call(
        kernel,
        out_shape=outs,
        in_specs=specs or [VMEM] * len(args),
        out_specs=jax.tree.map(lambda _: out_spec, outs),
        scratch_shapes=[pltpu.VMEM(dims, F32) if isinstance(dims, tuple) else dims for dims in scratch],
        input_output_aliases=aliases or {},
        compiler_params=pltpu.CompilerParams(vmem_limit_bytes=24 << 20, flags=FLAGS),
        cost_estimate=pl.CostEstimate(flops=flops, bytes_accessed=1 << 16, transcendentals=0),
        name=kernel.__name__,
    )(*args)


def per_device(mass, tracer, uvel, vvel, case_east, case_north, ice_blocks):
    ncat, height, width = mass.shape
    ncomp = tracer.shape[1] + 1
    nx, ny = lax.axis_size("gx"), lax.axis_size("gy")
    local = (mass, tracer, uvel, vvel, case_east, case_north)
    pairs = (ncat * ncomp + 4) // 2
    rows = height + 2 * PAD
    tall = FRONT + ncat * height + BACK
    block = FRONT + 32 * ncat + BACK
    deep = height + 3 * DEEP

    pay_a, pay_b, field, aux = call(
        pack_rows_kernel,
        tuple(pltpu.with_memory_space_constraint(x, pltpu.HBM) for x in (ice_blocks,) + local),
        (
            shape(pairs, 8, width),
            shape(pairs, 8, width),
            shape(ncomp, tall, width),
            shape(4, height + PAD, width),
        ),
        [
            pltpu.SMEM(ice_blocks.shape, jnp.int32),
            pltpu.VMEM((2, height, width), jnp.int32),
            pltpu.SemaphoreType.DMA((5 + 2 * ncat,)),
        ],
        1 << 20,
        specs=[HBM] * 7,
    )
    both = ("gx", "gy")
    pairs_a, pairs_b = [], []
    for j in range(ny):
        for i in range(nx):
            pairs_a.append((i * ny + j, i * ny + (j ^ 1)))
            if j == ny - 1:
                pairs_b.append((i * ny + j, (nx - 1 - i) * ny + j))
            elif j:
                pairs_b.append((i * ny + j, i * ny + (j + 1 if j % 2 else j - 1)))
    got_a = lax.ppermute(pay_a, both, pairs_a)
    got_b = lax.ppermute(pay_b, both, pairs_b)

    once, strips, geo = call(
        first_kernel,
        (field, aux),
        (shape(8, tall, width), shape(12, deep, width), shape(2, 7, rows, width)),
        [(8, 4, tall, width), (8, tall, width), (8, 8, width)],
        1 << 27,
    )
    halo, strips, pay_w, pay_e = call(
        pack_columns_kernel,
        (got_a, got_b, strips),
        (
            shape(2 * pairs, 16, width),
            shape(12, deep, width),
            shape(2, height + 2 * DEPTH, width),
            shape(2, height + 2 * DEPTH, width),
        ),
        [(2, pairs, 8, width), (pairs, 8, width)],
        1 << 20,
        aliases={2: 1},
    )
    ahead = [(i, (i + 1) % nx) for i in range(nx)]
    back = [(target, source) for source, target in ahead]
    got_w = lax.ppermute(pay_e, "gx", ahead)
    got_e = lax.ppermute(pay_w, "gx", back)
    (twice,) = call(
        second_kernel,
        (field, aux, once, geo, halo),
        (shape(8, tall, width),),
        [
            (2, 4, 40, width),
            (4, 40, width),
            (2, 2, 7, 40, width),
            (2, 7, 8, width),
            (8, block, width),
            (8, block, width),
            (8, 4, tall, width),
            (8, tall, width),
            (8, 8, width),
            (8, 8, width),
        ],
        1 << 27,
    )
    return call(
        finish_kernel,
        (strips, got_w, got_e, twice),
        (shape(ncat, height, width), shape(ncat, ncomp - 1, height, width)),
        [
            (12, deep, width),
            (4, 40, width),
            (2, 7, deep, width),
            (8, deep, width),
            (8, deep, width),
            (8, 4, deep, width),
            (8, deep, width),
            (8, 8, width),
            (ncat, 8, height, width),
            pltpu.SemaphoreType.DMA((2, ncat)),
        ],
        1 << 26,
        out_spec=HBM,
    )


def solution(mesh):
    placed = (
        P(None, "gy", "gx"),
        P(None, None, "gy", "gx"),
        P("gy", "gx"),
        P("gy", "gx"),
        P("gy", "gx"),
        P("gy", "gx"),
        P("gy", "gx"),
    )
    return jax.shard_map(
        per_device,
        mesh=mesh,
        in_specs=placed,
        out_specs=(P(None, "gy", "gx"), P(None, None, "gy", "gx")),
        check_vma=False,
    )
```

```python
import functools

import jax
import jax.numpy as jnp
from jax import lax
from jax.experimental import pallas as pl
from jax.experimental.pallas import tpu as pltpu
from jax.sharding import PartitionSpec as P

STEPS = 2
MASS_FLOOR = 0.1
FLAGS = {}
PAD = 8
DEEP = 16
FRONT = 16
BACK = 72
EARLY = 3
DEPTH = 2 * STEPS
STRIP = 6 * DEPTH
PER_PACK = STRIP // DEPTH
F32 = jnp.float32


def lanes_iota():
    return lax.broadcasted_iota(jnp.int32, (8, 128), 1)


def rows_iota():
    return lax.broadcasted_iota(jnp.int32, (8, 128), 0)


def roll(x, shift):
    return pltpu.roll(x, shift % 128 if isinstance(shift, int) else shift, 1)


def sel(mask, a, b):
    return jnp.where(mask, a, b)


def edge_geometry(speed, low, high, case):
    first = case == 1.0
    corner = sel(first, low, high)
    signs = sel(speed > 0.0, 1.0, -1.0)
    signed_area = sel(case == 0.0, 0.0, 0.5 * speed * corner)
    near = 0.25 * (signs - speed)
    far = 0.25 * signs - speed * (1.0 / 6.0)
    off = 0.25 - corner * (1.0 / 6.0)
    return speed, signed_area, near, far, off, sel(first, off, -off), case


def east_geometry(u, u_below, v, v_below, case):
    return edge_geometry(0.5 * (u + u_below), jnp.abs(v_below), jnp.abs(v), case)


def north_geometry(u, v, case):
    u_west, v_west = roll(u, 1), roll(v, 1)
    return edge_geometry(0.5 * (v + v_west), jnp.abs(u_west), jnp.abs(u), case)


def fill_geometry(geo, tiles, aux):
    for r in tiles:
        u, v = aux(0, r), aux(1, r)
        east = east_geometry(u, aux(0, r - 1), v, aux(1, r - 1), aux(2, r))
        north = north_geometry(u, v, aux(3, r))
        for n in range(7):
            geo[0, n, pl.ds(r, 8), :] = east[n]
            geo[1, n, pl.ds(r, 8), :] = north[n]


def ghost_aux(dst, src, base, top, height):
    for plane in range(4):
        dst[plane, pl.ds(0, 8), :] = src(plane, base)
    for r in (height - 8, height):
        at_fold = jnp.logical_and(top, rows_iota() + r >= height - 1)
        for plane in range(4):
            plain = src(plane, r)
            if plane < 2:
                ghost = -roll(src(plane, r + 1), -1)
            else:
                raw = roll(src(2, r), -1) if plane == 2 else src(3, r + 1)
                ghost = sel(raw == 0.0, 0.0, 3.0 - raw)
            dst[plane, pl.ds(r - base, 8), :] = sel(at_fold, ghost, plain)


def picks(low, high, low_slope, high_slope, forward, first):
    centre = sel(forward, low(0), high(0))
    slope = sel(forward, low_slope(0), high_slope(0))
    before = sel(forward, low(-1), high(-1))
    after = sel(forward, low(1), high(1))
    other_slope = sel(
        forward,
        sel(first, low_slope(-1), low_slope(1)),
        sel(first, high_slope(-1), high_slope(1)),
    )
    beyond = sel(forward, sel(first, low(-2), low(2)), sel(first, high(-2), high(2)))
    return centre, slope, before, after, other_slope, beyond


SLOPES = ("low", "high")


class Window:
    def __init__(self, load):
        self.load = load
        self.memo = {}

    def __call__(self, col, row):
        if (col, row) not in self.memo:
            self.memo[col, row] = self.load(col, row)
        return self.memo[col, row]


def picked(at, direction, masks):
    if direction == 0:
        return picks(
            lambda d: at(0, d),
            lambda d: at(1, d),
            lambda d: at("low", d),
            lambda d: at("high", d),
            *masks,
        )
    return picks(
        lambda d: at(d, 0),
        lambda d: at(d, 1),
        lambda d: at(d, 1) - at(d, -1),
        lambda d: at(d, 2) - at(d, 0),
        *masks,
    )


def mass_flux(geo, at, direction):
    speed, area, near, far, off, side, case = geo
    masks = (speed > 0.0, case == 1.0)
    centre, slope, before, after, other_slope, beyond = picked(at, direction, masks)
    first = masks[1]
    other = sel(first, before, after)
    w0 = speed * (centre + near * slope)
    w1 = area * (other + far * other_slope + off * (centre - beyond))
    w2 = area * (centre + far * slope + side * (before - after))
    w1_off = w1 * off
    w2_side = w2 * side
    weights = (
        w0 - w2 + w1_off,
        w0 * near - w2 * far,
        sel(first, w1, 0.0) - w2_side,
        sel(first, 0.0, w1) + w2_side,
        w1 * far,
        w1_off,
    )
    return w0 + w1 - w2, (masks, weights)


def tracer_flux(shared, at, direction):
    masks, weights = shared
    centre, slope, before, after, other_slope, beyond = picked(at, direction, masks)
    return (
        (weights[0] * centre + weights[1] * slope)
        + (weights[2] * before + weights[3] * after)
        + (weights[4] * other_slope - weights[5] * beyond)
    )


COLUMNS = (1, -1, 2, -2)
COPIES = 6


def rotations(value):
    return [roll(value, -col) for col in COLUMNS]


def keep_copies(shifted, k, row, value, moved):
    for n in range(4):
        shifted[k, n, pl.ds(row, 8), :] = moved[n]
    shifted[k, 4, pl.ds(row, 8), :] = moved[0] - moved[1]
    shifted[k, 5, pl.ds(row, 8), :] = moved[2] - value


def rotate_copies(source, shifted, row, k):
    value = source(k, row)
    keep_copies(shifted, k, row, value, rotations(value))


def window(source, shifted, k, row):
    def load(col, shift):
        if col == 0:
            return source(k, row + shift)
        n = COLUMNS.index(col) if col in COLUMNS else 4 + SLOPES.index(col)
        return shifted[k, n, pl.ds(row + shift, 8), :]

    return Window(load)


def north_alone(source, shifted, row, data):
    total, shared = mass_flux(data, window(source, shifted, 0, row), 1)
    out = [total]
    for k in range(1, 8):
        out.append(tracer_flux(shared, window(source, shifted, k, row), 1))
    return out


def run_tiles(count, start, stride, source, shifted, north, east, geometry, store, below=None, last_below=None, extra=None, spare=None, group=2):
    fresh_rows = (2,) if stride == 8 else (-2, 2)
    first_rows = {stride * j + r for j in range(group) for r in fresh_rows} | {-2, 2}
    for k in range(8):
        for r in sorted(first_rows):
            rotate_copies(source, shifted, start + r, k)

    def settle(i, k, row, rotated, mass, scale, lower=None):
        upper = north[k, pl.ds(row, 8), :]
        if lower is None:
            lower = north[k, pl.ds(row - 1, 8), :] if below is None else below[1][k]
        carried = mass if k == 0 else mass * source(k, row)
        fresh = (carried - upper + lower) - (east[k] - rotated)
        if k == 0:
            scale = 1.0 / jnp.maximum(fresh, MASS_FLOOR)
        else:
            fresh = fresh * scale
        store(k, i, row, fresh)
        return scale

    def tile(i):
        row = start + stride * i
        rotated = [roll(east[k], 1) for k in range(8)]
        copies = []
        for k in range(8):
            for fresh_row in fresh_rows:
                ahead = row + stride * group + fresh_row
                value = source(k, ahead)
                copies.append((k, ahead, value, rotations(value)))
        later = [extra(i, k, row) for k in range(8)] if extra else []
        at = window(source, shifted, 0, row)
        east_new, east_shared = mass_flux(geometry(0, i), at, 0)
        north_new, north_shared = mass_flux(geometry(1, i), at, 1)
        lower = north_alone(source, shifted, row - 1, below[0](i)) if below else None
        mass = source(0, row - stride)
        scale = None
        for k in range(8):
            if k:
                at = window(source, shifted, k, row)
                east_new = tracer_flux(east_shared, at, 0)
                north_new = tracer_flux(north_shared, at, 1)
            scale = settle(i - 1, k, row - stride, rotated[k], mass, scale)
            east[k] = east_new
            north[k, pl.ds(row, 8), :] = north_new
            if below:
                below[1][k] = lower[k]
        for k, ahead, value, moved in copies:
            keep_copies(shifted, k, ahead, value, moved)
        for finish in later:
            finish()

    def tiles(n, carry):
        for j in range(group):
            tile(n * group + j)
        return carry

    lax.fori_loop(0, count // group, tiles, 0)
    if spare is not None:
        spare[0, pl.ds(0, 8), :] = shifted[parity(), 0, pl.ds(8, 8), :]
    row = start + stride * (count - 1)
    rotated = [roll(east[k], 1) for k in range(8)]
    lower = north_alone(source, shifted, row - 1, last_below) if last_below else [None] * 8
    mass = source(0, row)
    scale = None
    for k in range(8):
        scale = settle(count - 1, k, row, rotated[k], mass, scale, lower[k])


def parity():
    return lax.rem(lax.axis_index("gy"), 2)


def at_fold_block():
    return lax.axis_index("gy") == lax.axis_size("gy") - 1


def pack_rows_kernel(ice, mass, tracer, u, v, ce, cn, pay_a, pay_b, field, aux, ice_s, ints, sems):
    ncat, height, width = mass.shape
    ncomp = tracer.shape[1] + 1
    block_rows, block_cols = ice.shape
    rows = pl.ds(PAD, height)
    pairs = [
        (ice, ice_s),
        (u, aux.at[0, rows, :]),
        (v, aux.at[1, rows, :]),
        (ce, ints.at[0]),
        (cn, ints.at[1]),
    ]
    for c in range(ncat):
        pairs.append((mass.at[c], field.at[0, pl.ds(FRONT + c * height, height), :]))
    for c in range(ncat):
        at = pl.ds(FRONT + c * height, height)
        pairs.append((tracer.at[c], field.at[pl.ds(1, ncomp - 1), at, :]))
    copies = [pltpu.make_async_copy(src, dst, sems.at[n]) for n, (src, dst) in enumerate(pairs)]
    for copy in copies:
        copy.start()
    for copy in copies[: 5 + ncat]:
        copy.wait()
    lane = lanes_iota()
    for n in range(2):
        for t in range(0, height, 8):
            aux[2 + n, pl.ds(PAD + t, 8), :] = ints[n, pl.ds(t, 8), :].astype(F32)
    for b in range(block_rows):
        tile = jnp.zeros((8, width), F32)
        for n in range(block_cols):
            inside = lane >= n * (width // block_cols)
            tile = sel(inside, ice_s[b, n].astype(F32), tile)
        for t in range(0, height // block_rows, 8):
            for c in range(ncat):
                at = pl.ds(FRONT + c * height + b * (height // block_rows) + t, 8)
                field[0, at, :] = field[0, at, :] * tile
    for copy in copies[5 + ncat :]:
        copy.wait()

    def write(dst, top):
        first = height - DEPTH if top else 0
        for p in range(ncat * ncomp + 4):
            c, k = divmod(p, ncomp)
            if c < ncat:
                value = field[k, pl.ds(FRONT + c * height + first, DEPTH), :]
            else:
                value = aux[k, pl.ds(PAD + first, DEPTH), :]
            half = (p % 2) ^ (1 if top else 0)
            dst[p // 2, pl.ds(DEPTH * half, DEPTH), :] = value

    @pl.when(parity() == 0)
    def _():
        write(pay_a, True)
        write(pay_b, False)

    @pl.when(parity() == 1)
    def _():
        write(pay_a, False)
        write(pay_b, True)


def first_kernel(field, aux, once, strips, geo, twice, shifted, north, east):
    height = aux.shape[1] - PAD
    ncat = (field.shape[1] - FRONT - BACK) // height
    per = height // 8
    lane = lanes_iota()
    fill_geometry(geo, range(PAD, PAD + height, 8), lambda n, r: aux[n, pl.ds(r, 8), :])
    where = strip_index(lane)
    for plane in range(4):
        for t in range(0, height, 8):
            strips[8 + plane, pl.ds(t + DEEP, 8), :] = gather(aux[plane, pl.ds(t + PAD, 8), :], where)

    def source(k, row):
        return field[k, pl.ds(row, 8), :]

    def geometry(direction, i):
        return [geo[direction, n, pl.ds(PAD + 8 * lax.rem(i, per), 8), :] for n in range(7)]

    def keep(k, i, row, value):
        once[k, pl.ds(row, 8), :] = value

    def place_strip(i, k, row):
        at = pl.ds(DEEP + 8 * lax.rem(i, per), 8)
        start = lax.div(i, per) * STRIP
        moved = gather(source(k, row), where)

        def finish():
            strips[k, at, :] = strip_merge(strips[k, at, :], moved, start, lane)

        return finish

    run_tiles(ncat * per, FRONT, 8, source, shifted, north, east, geometry, keep, extra=place_strip, spare=once, group=5)

    def middle(k, row):
        return once[k, pl.ds(row, 8), :]

    def keep_twice(k, i, row, value):
        twice[k, pl.ds(row, 8), :] = value

    start = FRONT + (ncat - EARLY) * height
    run_tiles(EARLY * per, start, 8, middle, shifted, north, east, geometry, keep_twice, spare=twice, group=4)


def gather(value, index):
    return jnp.take_along_axis(value, index, axis=1, mode="promise_in_bounds")


def strip_index(lane):
    at = lax.rem(lane, STRIP)
    index = sel(at < 3 * DEPTH, at - DEPTH, at + 128 - 5 * DEPTH)
    return jnp.clip(index, 0, 127)


def strip_merge(packed, moved, start, lane):
    at = lane - start
    return sel(jnp.logical_and(at >= DEPTH, at < 5 * DEPTH), moved, packed)


def pack_columns_kernel(got_a, got_b, strips_in, halo, strips, pay_w, pay_e, tmp, flip):
    height = strips.shape[1] - 3 * DEEP
    lane = lanes_iota()
    even = parity() == 0
    pairs = got_a.shape[0]
    for q in range(pairs):
        tmp[0, q] = sel(even, got_b[q], got_a[q])
        tmp[1, q] = sel(even, got_a[q], got_b[q])

    @pl.when(at_fold_block())
    def _():
        for q in range(pairs):
            flip[q] = gather(tmp[1, q], 127 - lane)
        for q in range(pairs):
            for s in range(8):
                tmp[1, q, pl.ds(s, 1), :] = flip[q, pl.ds(7 - s, 1), :]

    for p in range(2 * pairs):
        half = p % 2
        halo[p, pl.ds(PAD - DEPTH, DEPTH), :] = tmp[0, p // 2, pl.ds(DEPTH * (1 - half), DEPTH), :]
        halo[p, pl.ds(PAD, DEPTH), :] = tmp[1, p // 2, pl.ds(DEPTH * half, DEPTH), :]
    ncat = (2 * pairs - 4) // 8
    index = strip_index(lane)
    for k in range(12):
        for side in range(2):
            at = pl.ds(8 * side, 8)
            if k < 8:
                packed = jnp.zeros((8, 128), F32)
                for c in range(ncat):
                    packed = strip_merge(packed, gather(halo[8 * c + k, at, :], index), c * STRIP, lane)
            else:
                packed = gather(halo[8 * ncat + k - 8, at, :], index)
            strips[k, pl.ds(DEEP - 8 + side * (height + 8), 8), :] = packed
    where = lax.rem(lane, STRIP) // DEPTH
    for g in range(2):
        for t in range(0, height + 2 * DEPTH, 8):
            west = jnp.zeros((8, 128), F32)
            east = jnp.zeros((8, 128), F32)
            for n in range(PER_PACK):
                value = strips[PER_PACK * g + n, pl.ds(t + DEEP - DEPTH, 8), :]
                west = sel(where == n, roll(value, DEPTH * (n - 1)), west)
                east = sel(where == n, roll(value, DEPTH * (n - 4)), east)
            pay_w[g, pl.ds(t, 8), :] = west
            pay_e[g, pl.ds(t, 8), :] = east


def second_kernel(field, planes, once, geo_main, halo, twice_in, twice, aux, ghost, geo, south, edge, stage, shifted, north, east, held):
    height = planes.shape[1] - PAD
    ncat = (field.shape[1] - FRONT - BACK) // height
    per = height // 8
    own = ncat * 8

    def middle(k, row):
        return once[k, pl.ds(row, 8), :]

    def geometry(direction, i):
        return [geo_main[direction, n, pl.ds(PAD + 8 * lax.rem(i, per), 8), :] for n in range(7)]

    def keep(k, i, row, value):
        twice[k, pl.ds(row, 8), :] = value

    run_tiles(
        (ncat - EARLY) * per, FRONT, 8, middle, shifted, north, east, geometry, keep, group=4
    )

    for plane in range(4):
        aux[0, plane, pl.ds(0, 8), :] = halo[own + plane, pl.ds(0, 8), :]
        for n in range(2):
            aux[0, plane, pl.ds(8 + 8 * n, 8), :] = planes[plane, pl.ds(PAD + 8 * n, 8), :]
            aux[1, plane, pl.ds(8 * n, 8), :] = planes[plane, pl.ds(PAD + height - 16 + 8 * n, 8), :]
        aux[1, plane, pl.ds(16, 8), :] = halo[own + plane, pl.ds(8, 8), :]

    def low_aux(n, r):
        return aux[0, n, pl.ds(r, 8), :]

    def high_aux(n, r):
        return aux[1, n, pl.ds(r - height + 16, 8), :]

    def ghost_rows(n, r):
        return ghost[n, pl.ds(r, 8), :]

    ghost_aux(ghost, high_aux, height - 16, at_fold_block(), height)
    fill_geometry(geo.at[0], (3, 8), low_aux)
    fill_geometry(geo.at[1], (8,), lambda n, r: aux[1, n, pl.ds(r, 8), :])
    fill_geometry(geo.at[1], (16,), ghost_rows)
    for end, (src, r) in enumerate(((low_aux, 3), (ghost_rows, 11))):
        data = north_geometry(src(0, r), src(1, r), src(3, r))
        for n in range(7):
            south[end, n] = data[n]
    for c in range(ncat):
        base = FRONT + c * height
        at = FRONT + 32 * c
        for k in range(8):
            edge[k, pl.ds(at, 8), :] = halo[8 * c + k, pl.ds(0, 8), :]
            edge[k, pl.ds(at + 8, 8), :] = field[k, pl.ds(base, 8), :]
            edge[k, pl.ds(at + 16, 8), :] = field[k, pl.ds(base + height - 8, 8), :]
            edge[k, pl.ds(at + 24, 8), :] = halo[8 * c + k, pl.ds(8, 8), :]
            stage[k, pl.ds(at + 12, 8), :] = once[k, pl.ds(base + 4, 8), :]
            stage[k, pl.ds(at + 16, 8), :] = once[k, pl.ds(base + height - 14, 8), :]
            stage[k, pl.ds(at + 18, 8), :] = once[k, pl.ds(base + height - 12, 8), :]

    def end_of(i):
        return lax.rem(i + 2, 2)

    def edge_source(k, row):
        return edge[k, pl.ds(row, 8), :]

    def stage_source(k, row):
        return stage[k, pl.ds(row, 8), :]

    def edge_geometry_at(direction, i):
        end = end_of(i)
        return [geo[end, direction, n, pl.ds(4 + 8 * end, 8), :] for n in range(7)]

    def stage_geometry_at(direction, i):
        end = end_of(i)
        return [geo[end, direction, n, pl.ds(7 + 2 * end, 8), :] for n in range(7)]

    def south_at(i):
        end = end_of(i)
        return [south[end, n] for n in range(7)]

    def keep_stage(k, i, row, value):
        stage[k, pl.ds(row + 6 * end_of(i), 8), :] = value

    inside = jnp.logical_and(rows_iota() >= 1, rows_iota() <= 6)

    def keep_rim(k, i, row, value):
        c = lax.div(i + 2, 2) - 1
        at = pl.ds(FRONT + height * c - 1 + (height - 6) * end_of(i), 8)
        twice[k, at, :] = sel(inside, value, twice[k, at, :])

    run_tiles(
        2 * ncat, FRONT + 4, 16, edge_source, shifted, north, east, edge_geometry_at, keep_stage, below=(south_at, held)
    )
    run_tiles(2 * ncat, FRONT + 7, 16, stage_source, shifted, north, east, stage_geometry_at, keep_rim, spare=twice)


def finish_kernel(strips_in, got_w, got_e, twice, mass_out, tracer_out, strips, ghost, geo, stage, last, shifted, north, east, whole, sems):
    ncat, height, width = mass_out.shape
    lane = lanes_iota()
    at = lax.rem(lane, STRIP)
    for k in range(12):
        g, n = divmod(k, PER_PACK)
        for t in range(0, height + 2 * DEPTH, 8):
            value = strips_in[k, pl.ds(t + DEEP - DEPTH, 8), :]
            value = sel(at < DEPTH, roll(got_w[g, pl.ds(t, 8), :], -DEPTH * n), value)
            value = sel(at >= 5 * DEPTH, roll(got_e[g, pl.ds(t, 8), :], DEPTH * (5 - n)), value)
            strips[k, pl.ds(t + DEEP - DEPTH, 8), :] = value

    def aux(n, r):
        return strips[8 + n, pl.ds(r, 8), :]

    def ghost_rows(n, r):
        return ghost[n, pl.ds(r - (height - 16 + DEEP), 8), :]

    ghost_aux(ghost, lambda n, r: aux(n, r + DEEP), height - 16, at_fold_block(), height)
    fill_geometry(geo, [DEEP - 4] + list(range(DEEP, DEEP + height, 8)), aux)
    fill_geometry(geo, (DEEP + height,), ghost_rows)
    south = north_geometry(*(ghost_rows(n, DEEP + height - 5) for n in (0, 1, 3)))

    def source(k, row):
        return strips[k, pl.ds(row, 8), :]

    def middle(k, row):
        return stage[k, pl.ds(row, 8), :]

    def keep(k, i, row, value):
        stage[k, pl.ds(row, 8), :] = value

    def keep_last(k, i, row, value):
        last[k, pl.ds(row, 8), :] = value

    def geometry(direction, i):
        return [geo[direction, n, pl.ds(DEEP - 4 + 8 * i, 8), :] for n in range(7)]

    count = height // 8 + 1
    run_tiles(count, DEEP - 4, 8, source, shifted, north, east, geometry, keep, last_below=south, group=3)
    run_tiles(count, DEEP - 4, 8, middle, shifted, north, east, geometry, keep_last, group=3)

    def out_copies(c):
        return (
            pltpu.make_async_copy(whole.at[c, 0], mass_out.at[c], sems.at[0, c]),
            pltpu.make_async_copy(whole.at[c, pl.ds(1, 7)], tracer_out.at[c], sems.at[1, c]),
        )

    edges = jnp.logical_or(lane < DEPTH, lane >= 128 - DEPTH)
    for c in range(ncat):
        index = sel(lane < 64, lane + DEPTH, lane - 128 + 5 * DEPTH) + c * STRIP
        index = jnp.clip(index, 0, 127)
        for k in range(8):
            for t in range(0, height, 8):
                value = twice[k, pl.ds(FRONT + c * height + t, 8), :]
                moved = gather(last[k, pl.ds(t + DEEP, 8), :], index)
                whole[c, k, pl.ds(t, 8), :] = sel(edges, moved, value)
        if c:
            for copy in out_copies(c - 1):
                copy.start()
    for copy in out_copies(ncat - 1):
        copy.start()
    for c in range(ncat):
        for copy in out_copies(c):
            copy.wait()


def shape(*dims):
    return jax.ShapeDtypeStruct(dims, F32)


VMEM = pl.BlockSpec(memory_space=pltpu.VMEM)
HBM = pl.BlockSpec(memory_space=pltpu.HBM)


def call(kernel, args, outs, scratch, flops, aliases=None, specs=None, out_spec=VMEM):
    return pl.pallas_call(
        kernel,
        out_shape=outs,
        in_specs=specs or [VMEM] * len(args),
        out_specs=jax.tree.map(lambda _: out_spec, outs),
        scratch_shapes=[pltpu.VMEM(dims, F32) if isinstance(dims, tuple) else dims for dims in scratch],
        input_output_aliases=aliases or {},
        compiler_params=pltpu.CompilerParams(vmem_limit_bytes=24 << 20, flags=FLAGS),
        cost_estimate=pl.CostEstimate(flops=flops, bytes_accessed=1 << 16, transcendentals=0),
        name=kernel.__name__,
    )(*args)


def per_device(mass, tracer, uvel, vvel, case_east, case_north, ice_blocks):
    ncat, height, width = mass.shape
    ncomp = tracer.shape[1] + 1
    nx, ny = lax.axis_size("gx"), lax.axis_size("gy")
    local = (mass, tracer, uvel, vvel, case_east, case_north)
    pairs = (ncat * ncomp + 4) // 2
    rows = height + 2 * PAD
    tall = FRONT + ncat * height + BACK
    block = FRONT + 32 * ncat + BACK
    deep = height + 3 * DEEP

    pay_a, pay_b, field, aux = call(
        pack_rows_kernel,
        tuple(pltpu.with_memory_space_constraint(x, pltpu.HBM) for x in (ice_blocks,) + local),
        (
            shape(pairs, 8, width),
            shape(pairs, 8, width),
            shape(ncomp, tall, width),
            shape(4, height + PAD, width),
        ),
        [
            pltpu.SMEM(ice_blocks.shape, jnp.int32),
            pltpu.VMEM((2, height, width), jnp.int32),
            pltpu.SemaphoreType.DMA((5 + 2 * ncat,)),
        ],
        1 << 20,
        specs=[HBM] * 7,
    )
    both = ("gx", "gy")
    pairs_a, pairs_b = [], []
    for j in range(ny):
        for i in range(nx):
            pairs_a.append((i * ny + j, i * ny + (j ^ 1)))
            if j == ny - 1:
                pairs_b.append((i * ny + j, (nx - 1 - i) * ny + j))
            elif j:
                pairs_b.append((i * ny + j, i * ny + (j + 1 if j % 2 else j - 1)))
    got_a = lax.ppermute(pay_a, both, pairs_a)
    got_b = lax.ppermute(pay_b, both, pairs_b)

    once, strips, geo, twice = call(
        first_kernel,
        (field, aux),
        (shape(8, tall, width), shape(12, deep, width), shape(2, 7, rows, width), shape(8, tall, width)),
        [(8, COPIES, tall, width), (8, tall, width), (8, 8, width)],
        1 << 27,
    )
    halo, strips, pay_w, pay_e = call(
        pack_columns_kernel,
        (got_a, got_b, strips),
        (
            shape(2 * pairs, 16, width),
            shape(12, deep, width),
            shape(2, height + 2 * DEPTH, width),
            shape(2, height + 2 * DEPTH, width),
        ),
        [(2, pairs, 8, width), (pairs, 8, width)],
        1 << 20,
        aliases={2: 1},
    )
    ahead = [(i, (i + 1) % nx) for i in range(nx)]
    back = [(target, source) for source, target in ahead]
    got_w = lax.ppermute(pay_e, "gx", ahead)
    got_e = lax.ppermute(pay_w, "gx", back)
    (twice,) = call(
        second_kernel,
        (field, aux, once, geo, halo, twice),
        (shape(8, tall, width),),
        [
            (2, 4, 40, width),
            (4, 40, width),
            (2, 2, 7, 40, width),
            (2, 7, 8, width),
            (8, block, width),
            (8, block, width),
            (8, COPIES, tall, width),
            (8, tall, width),
            (8, 8, width),
            (8, 8, width),
        ],
        1 << 27,
        aliases={5: 0},
    )
    return call(
        finish_kernel,
        (strips, got_w, got_e, twice),
        (shape(ncat, height, width), shape(ncat, ncomp - 1, height, width)),
        [
            (12, deep, width),
            (4, 40, width),
            (2, 7, deep, width),
            (8, deep, width),
            (8, deep, width),
            (8, COPIES, deep, width),
            (8, deep, width),
            (8, 8, width),
            (ncat, 8, height, width),
            pltpu.SemaphoreType.DMA((2, ncat)),
        ],
        1 << 26,
        out_spec=HBM,
    )


def solution(mesh):
    placed = (
        P(None, "gy", "gx"),
        P(None, None, "gy", "gx"),
        P("gy", "gx"),
        P("gy", "gx"),
        P("gy", "gx"),
        P("gy", "gx"),
        P("gy", "gx"),
    )
    return jax.shard_map(
        per_device,
        mesh=mesh,
        in_specs=placed,
        out_specs=(P(None, "gy", "gx"), P(None, None, "gy", "gx")),
        check_vma=False,
    )
```

```python
import functools

import jax
import jax.numpy as jnp
from jax import lax
from jax.experimental import pallas as pl
from jax.experimental.pallas import tpu as pltpu
from jax.sharding import PartitionSpec as P

STEPS = 2
MASS_FLOOR = 0.1
FLAGS = {}
PAD = 8
DEEP = 16
FRONT = 16
BACK = 72
DEPTH = 2 * STEPS
STRIP = 6 * DEPTH
PER_PACK = STRIP // DEPTH
F32 = jnp.float32


def lanes_iota():
    return lax.broadcasted_iota(jnp.int32, (8, 128), 1)


def rows_iota():
    return lax.broadcasted_iota(jnp.int32, (8, 128), 0)


def roll(x, shift):
    return pltpu.roll(x, shift % 128 if isinstance(shift, int) else shift, 1)


def sel(mask, a, b):
    return jnp.where(mask, a, b)


def edge_geometry(speed, low, high, case):
    first = case == 1.0
    corner = sel(first, low, high)
    signs = sel(speed > 0.0, 1.0, -1.0)
    signed_area = sel(case == 0.0, 0.0, 0.5 * speed * corner)
    near = 0.25 * (signs - speed)
    far = 0.25 * signs - speed * (1.0 / 6.0)
    off = 0.25 - corner * (1.0 / 6.0)
    return speed, signed_area, near, far, off, sel(first, off, -off), case


def east_geometry(u, u_below, v, v_below, case):
    return edge_geometry(0.5 * (u + u_below), jnp.abs(v_below), jnp.abs(v), case)


def north_geometry(u, v, case):
    u_west, v_west = roll(u, 1), roll(v, 1)
    return edge_geometry(0.5 * (v + v_west), jnp.abs(u_west), jnp.abs(u), case)


def fill_geometry(geo, tiles, aux):
    for r in tiles:
        u, v = aux(0, r), aux(1, r)
        east = east_geometry(u, aux(0, r - 1), v, aux(1, r - 1), aux(2, r))
        north = north_geometry(u, v, aux(3, r))
        for n in range(7):
            geo[0, n, pl.ds(r, 8), :] = east[n]
            geo[1, n, pl.ds(r, 8), :] = north[n]


def ghost_aux(dst, src, base, top, height):
    for plane in range(4):
        dst[plane, pl.ds(0, 8), :] = src(plane, base)
    for r in (height - 8, height):
        at_fold = jnp.logical_and(top, rows_iota() + r >= height - 1)
        for plane in range(4):
            plain = src(plane, r)
            if plane < 2:
                ghost = -roll(src(plane, r + 1), -1)
            else:
                raw = roll(src(2, r), -1) if plane == 2 else src(3, r + 1)
                ghost = sel(raw == 0.0, 0.0, 3.0 - raw)
            dst[plane, pl.ds(r - base, 8), :] = sel(at_fold, ghost, plain)


def picks(low, high, low_slope, high_slope, forward, first):
    centre = sel(forward, low(0), high(0))
    slope = sel(forward, low_slope(0), high_slope(0))
    before = sel(forward, low(-1), high(-1))
    after = sel(forward, low(1), high(1))
    other_slope = sel(
        forward,
        sel(first, low_slope(-1), low_slope(1)),
        sel(first, high_slope(-1), high_slope(1)),
    )
    beyond = sel(forward, sel(first, low(-2), low(2)), sel(first, high(-2), high(2)))
    return centre, slope, before, after, other_slope, beyond


class Window:
    def __init__(self, load):
        self.load = load
        self.memo = {}

    def __call__(self, col, row):
        if (col, row) not in self.memo:
            self.memo[col, row] = self.load(col, row)
        return self.memo[col, row]


def picked(at, direction, masks):
    if direction == 0:
        return picks(
            lambda d: at(0, d),
            lambda d: at(1, d),
            lambda d: at(1, d) - at(-1, d),
            lambda d: at(2, d) - at(0, d),
            *masks,
        )
    return picks(
        lambda d: at(d, 0),
        lambda d: at(d, 1),
        lambda d: at(d, 1) - at(d, -1),
        lambda d: at(d, 2) - at(d, 0),
        *masks,
    )


def mass_flux(geo, at, direction):
    speed, area, near, far, off, side, case = geo
    masks = (speed > 0.0, case == 1.0)
    centre, slope, before, after, other_slope, beyond = picked(at, direction, masks)
    first = masks[1]
    other = sel(first, before, after)
    w0 = speed * (centre + near * slope)
    w1 = area * (other + far * other_slope + off * (centre - beyond))
    w2 = area * (centre + far * slope + side * (before - after))
    w1_off = w1 * off
    w2_side = w2 * side
    weights = (
        w0 - w2 + w1_off,
        w0 * near - w2 * far,
        sel(first, w1, 0.0) - w2_side,
        sel(first, 0.0, w1) + w2_side,
        w1 * far,
        w1_off,
    )
    return w0 + w1 - w2, (masks, weights)


def tracer_flux(shared, at, direction):
    masks, weights = shared
    centre, slope, before, after, other_slope, beyond = picked(at, direction, masks)
    return (
        (weights[0] * centre + weights[1] * slope)
        + (weights[2] * before + weights[3] * after)
        + (weights[4] * other_slope - weights[5] * beyond)
    )


COLUMNS = (1, -1, 2, -2)


def rotate_copies(source, shifted, row, k):
    value = source(k, row)
    for n, col in enumerate(COLUMNS):
        shifted[k, n, pl.ds(row, 8), :] = roll(value, -col)


def window(source, shifted, k, row):
    def load(col, shift):
        if col == 0:
            return source(k, row + shift)
        return shifted[k, COLUMNS.index(col), pl.ds(row + shift, 8), :]

    return Window(load)


def north_alone(source, shifted, row, data):
    total, shared = mass_flux(data, window(source, shifted, 0, row), 1)
    out = [total]
    for k in range(1, 8):
        out.append(tracer_flux(shared, window(source, shifted, k, row), 1))
    return out


def run_tiles(count, start, stride, source, shifted, north, east, geometry, store, below=None, last_below=None, extra=None, spare=None, group=2):
    fresh_rows = (2,) if stride == 8 else (-2, 2)
    first_rows = {stride * j + r for j in range(group) for r in fresh_rows} | {-2, 2}
    for k in range(8):
        for r in sorted(first_rows):
            rotate_copies(source, shifted, start + r, k)

    def settle(i, k, row, rotated, mass, scale, lower=None):
        upper = north[k, pl.ds(row, 8), :]
        if lower is None:
            lower = north[k, pl.ds(row - 1, 8), :] if below is None else below[1][k]
        carried = mass if k == 0 else mass * source(k, row)
        fresh = (carried - upper + lower) - (east[k] - rotated)
        if k == 0:
            scale = 1.0 / jnp.maximum(fresh, MASS_FLOOR)
        else:
            fresh = fresh * scale
        store(k, i, row, fresh)
        return scale

    def tile(i):
        row = start + stride * i
        rotated = [roll(east[k], 1) for k in range(8)]
        copies = []
        for k in range(8):
            for fresh_row in fresh_rows:
                ahead = row + stride * group + fresh_row
                value = source(k, ahead)
                copies.append((k, ahead, [roll(value, -col) for col in COLUMNS]))
        later = [extra(i, k, row) for k in range(8)] if extra else []
        at = window(source, shifted, 0, row)
        east_new, east_shared = mass_flux(geometry(0, i), at, 0)
        north_new, north_shared = mass_flux(geometry(1, i), at, 1)
        lower = north_alone(source, shifted, row - 1, below[0](i)) if below else None
        mass = source(0, row - stride)
        scale = None
        for k in range(8):
            if k:
                at = window(source, shifted, k, row)
                east_new = tracer_flux(east_shared, at, 0)
                north_new = tracer_flux(north_shared, at, 1)
            scale = settle(i - 1, k, row - stride, rotated[k], mass, scale)
            east[k] = east_new
            north[k, pl.ds(row, 8), :] = north_new
            if below:
                below[1][k] = lower[k]
        for k, ahead, moved in copies:
            for n in range(4):
                shifted[k, n, pl.ds(ahead, 8), :] = moved[n]
        for finish in later:
            finish()

    def tiles(n, carry):
        for j in range(group):
            tile(n * group + j)
        return carry

    lax.fori_loop(0, count // group, tiles, 0)
    if spare is not None:
        spare[0, pl.ds(0, 8), :] = shifted[parity(), 0, pl.ds(8, 8), :]
    row = start + stride * (count - 1)
    rotated = [roll(east[k], 1) for k in range(8)]
    lower = north_alone(source, shifted, row - 1, last_below) if last_below else [None] * 8
    mass = source(0, row)
    scale = None
    for k in range(8):
        scale = settle(count - 1, k, row, rotated[k], mass, scale, lower[k])


def parity():
    return lax.rem(lax.axis_index("gy"), 2)


def even_column():
    return lax.rem(lax.axis_index("gx"), 2) == 0


def at_fold_block():
    return lax.axis_index("gy") == lax.axis_size("gy") - 1


def pack_rows_kernel(ice, mass, tracer, u, v, ce, cn, pay_a, pay_b, field, aux, ice_s, ints, sems):
    ncat, height, width = mass.shape
    ncomp = tracer.shape[1] + 1
    block_rows, block_cols = ice.shape
    rows = pl.ds(PAD, height)
    pairs = [
        (ice, ice_s),
        (u, aux.at[0, rows, :]),
        (v, aux.at[1, rows, :]),
        (ce, ints.at[0]),
        (cn, ints.at[1]),
    ]
    for c in range(ncat):
        pairs.append((mass.at[c], field.at[0, pl.ds(FRONT + c * height, height), :]))
    for c in range(ncat):
        at = pl.ds(FRONT + c * height, height)
        pairs.append((tracer.at[c], field.at[pl.ds(1, ncomp - 1), at, :]))
    copies = [pltpu.make_async_copy(src, dst, sems.at[n]) for n, (src, dst) in enumerate(pairs)]
    for copy in copies:
        copy.start()
    for copy in copies[: 5 + ncat]:
        copy.wait()
    lane = lanes_iota()
    for n in range(2):
        for t in range(0, height, 8):
            aux[2 + n, pl.ds(PAD + t, 8), :] = ints[n, pl.ds(t, 8), :].astype(F32)
    for b in range(block_rows):
        tile = jnp.zeros((8, width), F32)
        for n in range(block_cols):
            inside = lane >= n * (width // block_cols)
            tile = sel(inside, ice_s[b, n].astype(F32), tile)
        for t in range(0, height // block_rows, 8):
            for c in range(ncat):
                at = pl.ds(FRONT + c * height + b * (height // block_rows) + t, 8)
                field[0, at, :] = field[0, at, :] * tile
    for copy in copies[5 + ncat :]:
        copy.wait()

    def write(dst, top):
        first = height - DEPTH if top else 0
        for p in range(ncat * ncomp + 4):
            c, k = divmod(p, ncomp)
            if c < ncat:
                value = field[k, pl.ds(FRONT + c * height + first, DEPTH), :]
            else:
                value = aux[k, pl.ds(PAD + first, DEPTH), :]
            half = (p % 2) ^ (1 if top else 0)
            dst[p // 2, pl.ds(DEPTH * half, DEPTH), :] = value

    @pl.when(parity() == 0)
    def _():
        write(pay_a, True)
        write(pay_b, False)

    @pl.when(parity() == 1)
    def _():
        write(pay_a, False)
        write(pay_b, True)


def first_kernel(field, aux, once, strips, geo, shifted, north, east):
    height = aux.shape[1] - PAD
    ncat = (field.shape[1] - FRONT - BACK) // height
    per = height // 8
    lane = lanes_iota()
    fill_geometry(geo, range(PAD, PAD + height, 8), lambda n, r: aux[n, pl.ds(r, 8), :])
    where = strip_index(lane)
    for plane in range(4):
        for t in range(0, height, 8):
            strips[8 + plane, pl.ds(t + DEEP, 8), :] = gather(aux[plane, pl.ds(t + PAD, 8), :], where)

    def source(k, row):
        return field[k, pl.ds(row, 8), :]

    def geometry(direction, i):
        return [geo[direction, n, pl.ds(PAD + 8 * lax.rem(i, per), 8), :] for n in range(7)]

    def keep(k, i, row, value):
        once[k, pl.ds(row, 8), :] = value

    def place_strip(i, k, row):
        at = pl.ds(DEEP + 8 * lax.rem(i, per), 8)
        start = lax.div(i, per) * STRIP
        moved = gather(source(k, row), where)

        def finish():
            strips[k, at, :] = strip_merge(strips[k, at, :], moved, start, lane)

        return finish

    run_tiles(ncat * per, FRONT, 8, source, shifted, north, east, geometry, keep, extra=place_strip, spare=once, group=5)


def gather(value, index):
    return jnp.take_along_axis(value, index, axis=1, mode="promise_in_bounds")


def strip_index(lane):
    at = lax.rem(lane, STRIP)
    index = sel(at < 3 * DEPTH, at - DEPTH, at + 128 - 5 * DEPTH)
    return jnp.clip(index, 0, 127)


def strip_merge(packed, moved, start, lane):
    at = lane - start
    return sel(jnp.logical_and(at >= DEPTH, at < 5 * DEPTH), moved, packed)


def pack_columns_kernel(got_a, got_b, strips_in, halo, strips, pay_c, pay_d, tmp, flip):
    height = strips.shape[1] - 3 * DEEP
    lane = lanes_iota()
    even = parity() == 0
    pairs = got_a.shape[0]
    for q in range(pairs):
        tmp[0, q] = sel(even, got_b[q], got_a[q])
        tmp[1, q] = sel(even, got_a[q], got_b[q])

    @pl.when(at_fold_block())
    def _():
        for q in range(pairs):
            flip[q] = gather(tmp[1, q], 127 - lane)
        for q in range(pairs):
            for s in range(8):
                tmp[1, q, pl.ds(s, 1), :] = flip[q, pl.ds(7 - s, 1), :]

    for p in range(2 * pairs):
        half = p % 2
        halo[p, pl.ds(PAD - DEPTH, DEPTH), :] = tmp[0, p // 2, pl.ds(DEPTH * (1 - half), DEPTH), :]
        halo[p, pl.ds(PAD, DEPTH), :] = tmp[1, p // 2, pl.ds(DEPTH * half, DEPTH), :]
    ncat = (2 * pairs - 4) // 8
    index = strip_index(lane)
    for k in range(12):
        for side in range(2):
            at = pl.ds(8 * side, 8)
            if k < 8:
                packed = jnp.zeros((8, 128), F32)
                for c in range(ncat):
                    packed = strip_merge(packed, gather(halo[8 * c + k, at, :], index), c * STRIP, lane)
            else:
                packed = gather(halo[8 * ncat + k - 8, at, :], index)
            strips[k, pl.ds(DEEP - 8 + side * (height + 8), 8), :] = packed
    where = lax.rem(lane, STRIP) // DEPTH
    for g in range(2):
        for t in range(0, height + 2 * DEPTH, 8):
            west = jnp.zeros((8, 128), F32)
            east = jnp.zeros((8, 128), F32)
            for n in range(PER_PACK):
                value = strips[PER_PACK * g + n, pl.ds(t + DEEP - DEPTH, 8), :]
                west = sel(where == n, roll(value, DEPTH * (n - 1)), west)
                east = sel(where == n, roll(value, DEPTH * (n - 4)), east)
            pay_c[g, pl.ds(t, 8), :] = sel(even_column(), east, west)
            pay_d[g, pl.ds(t, 8), :] = sel(even_column(), west, east)


def second_kernel(field, planes, once, geo_main, halo, twice, aux, ghost, geo, south, edge, stage, shifted, north, east, held):
    height = planes.shape[1] - PAD
    ncat = (field.shape[1] - FRONT - BACK) // height
    per = height // 8
    own = ncat * 8

    def middle(k, row):
        return once[k, pl.ds(row, 8), :]

    def geometry(direction, i):
        return [geo_main[direction, n, pl.ds(PAD + 8 * lax.rem(i, per), 8), :] for n in range(7)]

    def keep(k, i, row, value):
        twice[k, pl.ds(row, 8), :] = value

    run_tiles(ncat * per, FRONT, 8, middle, shifted, north, east, geometry, keep, group=5)

    for plane in range(4):
        aux[0, plane, pl.ds(0, 8), :] = halo[own + plane, pl.ds(0, 8), :]
        for n in range(2):
            aux[0, plane, pl.ds(8 + 8 * n, 8), :] = planes[plane, pl.ds(PAD + 8 * n, 8), :]
            aux[1, plane, pl.ds(8 * n, 8), :] = planes[plane, pl.ds(PAD + height - 16 + 8 * n, 8), :]
        aux[1, plane, pl.ds(16, 8), :] = halo[own + plane, pl.ds(8, 8), :]

    def low_aux(n, r):
        return aux[0, n, pl.ds(r, 8), :]

    def high_aux(n, r):
        return aux[1, n, pl.ds(r - height + 16, 8), :]

    def ghost_rows(n, r):
        return ghost[n, pl.ds(r, 8), :]

    ghost_aux(ghost, high_aux, height - 16, at_fold_block(), height)
    fill_geometry(geo.at[0], (3, 8), low_aux)
    fill_geometry(geo.at[1], (8,), lambda n, r: aux[1, n, pl.ds(r, 8), :])
    fill_geometry(geo.at[1], (16,), ghost_rows)
    for end, (src, r) in enumerate(((low_aux, 3), (ghost_rows, 11))):
        data = north_geometry(src(0, r), src(1, r), src(3, r))
        for n in range(7):
            south[end, n] = data[n]
    for c in range(ncat):
        base = FRONT + c * height
        at = FRONT + 32 * c
        for k in range(8):
            edge[k, pl.ds(at, 8), :] = halo[8 * c + k, pl.ds(0, 8), :]
            edge[k, pl.ds(at + 8, 8), :] = field[k, pl.ds(base, 8), :]
            edge[k, pl.ds(at + 16, 8), :] = field[k, pl.ds(base + height - 8, 8), :]
            edge[k, pl.ds(at + 24, 8), :] = halo[8 * c + k, pl.ds(8, 8), :]
            stage[k, pl.ds(at + 12, 8), :] = once[k, pl.ds(base + 4, 8), :]
            stage[k, pl.ds(at + 16, 8), :] = once[k, pl.ds(base + height - 14, 8), :]
            stage[k, pl.ds(at + 18, 8), :] = once[k, pl.ds(base + height - 12, 8), :]

    def end_of(i):
        return lax.rem(i + 2, 2)

    def edge_source(k, row):
        return edge[k, pl.ds(row, 8), :]

    def stage_source(k, row):
        return stage[k, pl.ds(row, 8), :]

    def edge_geometry_at(direction, i):
        end = end_of(i)
        return [geo[end, direction, n, pl.ds(4 + 8 * end, 8), :] for n in range(7)]

    def stage_geometry_at(direction, i):
        end = end_of(i)
        return [geo[end, direction, n, pl.ds(7 + 2 * end, 8), :] for n in range(7)]

    def south_at(i):
        end = end_of(i)
        return [south[end, n] for n in range(7)]

    def keep_stage(k, i, row, value):
        stage[k, pl.ds(row + 6 * end_of(i), 8), :] = value

    inside = jnp.logical_and(rows_iota() >= 1, rows_iota() <= 6)

    def keep_rim(k, i, row, value):
        c = lax.div(i + 2, 2) - 1
        at = pl.ds(FRONT + height * c - 1 + (height - 6) * end_of(i), 8)
        twice[k, at, :] = sel(inside, value, twice[k, at, :])

    run_tiles(
        2 * ncat, FRONT + 4, 16, edge_source, shifted, north, east, edge_geometry_at, keep_stage, below=(south_at, held)
    )
    run_tiles(2 * ncat, FRONT + 7, 16, stage_source, shifted, north, east, stage_geometry_at, keep_rim, spare=twice)


def finish_kernel(strips_in, got_c, got_d, twice, mass_out, tracer_out, got, strips, ghost, geo, stage, last, shifted, north, east, whole, sems):
    ncat, height, width = mass_out.shape
    lane = lanes_iota()
    at = lax.rem(lane, STRIP)
    for g in range(2):
        for t in range(0, height + 2 * DEPTH, 8):
            inner, outer = got_c[g, pl.ds(t, 8), :], got_d[g, pl.ds(t, 8), :]
            got[0, g, pl.ds(t, 8), :] = sel(even_column(), outer, inner)
            got[1, g, pl.ds(t, 8), :] = sel(even_column(), inner, outer)
    for k in range(12):
        g, n = divmod(k, PER_PACK)
        for t in range(0, height + 2 * DEPTH, 8):
            value = strips_in[k, pl.ds(t + DEEP - DEPTH, 8), :]
            value = sel(at < DEPTH, roll(got[0, g, pl.ds(t, 8), :], -DEPTH * n), value)
            value = sel(at >= 5 * DEPTH, roll(got[1, g, pl.ds(t, 8), :], DEPTH * (5 - n)), value)
            strips[k, pl.ds(t + DEEP - DEPTH, 8), :] = value

    def aux(n, r):
        return strips[8 + n, pl.ds(r, 8), :]

    def ghost_rows(n, r):
        return ghost[n, pl.ds(r - (height - 16 + DEEP), 8), :]

    ghost_aux(ghost, lambda n, r: aux(n, r + DEEP), height - 16, at_fold_block(), height)
    fill_geometry(geo, [DEEP - 4] + list(range(DEEP, DEEP + height, 8)), aux)
    fill_geometry(geo, (DEEP + height,), ghost_rows)
    south = north_geometry(*(ghost_rows(n, DEEP + height - 5) for n in (0, 1, 3)))

    def source(k, row):
        return strips[k, pl.ds(row, 8), :]

    def middle(k, row):
        return stage[k, pl.ds(row, 8), :]

    def keep(k, i, row, value):
        stage[k, pl.ds(row, 8), :] = value

    def keep_last(k, i, row, value):
        last[k, pl.ds(row, 8), :] = value

    def geometry(direction, i):
        return [geo[direction, n, pl.ds(DEEP - 4 + 8 * i, 8), :] for n in range(7)]

    count = height // 8 + 1
    run_tiles(count, DEEP - 4, 8, source, shifted, north, east, geometry, keep, last_below=south, group=3)
    run_tiles(count, DEEP - 4, 8, middle, shifted, north, east, geometry, keep_last, group=3)

    def out_copies(c):
        return (
            pltpu.make_async_copy(whole.at[c, 0], mass_out.at[c], sems.at[0, c]),
            pltpu.make_async_copy(whole.at[c, pl.ds(1, 7)], tracer_out.at[c], sems.at[1, c]),
        )

    edges = jnp.logical_or(lane < DEPTH, lane >= 128 - DEPTH)
    for c in range(ncat):
        index = sel(lane < 64, lane + DEPTH, lane - 128 + 5 * DEPTH) + c * STRIP
        index = jnp.clip(index, 0, 127)
        for k in range(8):
            for t in range(0, height, 8):
                value = twice[k, pl.ds(FRONT + c * height + t, 8), :]
                moved = gather(last[k, pl.ds(t + DEEP, 8), :], index)
                whole[c, k, pl.ds(t, 8), :] = sel(edges, moved, value)
        if c:
            for copy in out_copies(c - 1):
                copy.start()
    for copy in out_copies(ncat - 1):
        copy.start()
    for c in range(ncat):
        for copy in out_copies(c):
            copy.wait()


def shape(*dims):
    return jax.ShapeDtypeStruct(dims, F32)


VMEM = pl.BlockSpec(memory_space=pltpu.VMEM)
HBM = pl.BlockSpec(memory_space=pltpu.HBM)


def call(kernel, args, outs, scratch, flops, aliases=None, specs=None, out_spec=VMEM):
    return pl.pallas_call(
        kernel,
        out_shape=outs,
        in_specs=specs or [VMEM] * len(args),
        out_specs=jax.tree.map(lambda _: out_spec, outs),
        scratch_shapes=[pltpu.VMEM(dims, F32) if isinstance(dims, tuple) else dims for dims in scratch],
        input_output_aliases=aliases or {},
        compiler_params=pltpu.CompilerParams(vmem_limit_bytes=24 << 20, flags=FLAGS),
        cost_estimate=pl.CostEstimate(flops=flops, bytes_accessed=1 << 16, transcendentals=0),
        name=kernel.__name__,
    )(*args)


def per_device(mass, tracer, uvel, vvel, case_east, case_north, ice_blocks):
    ncat, height, width = mass.shape
    ncomp = tracer.shape[1] + 1
    nx, ny = lax.axis_size("gx"), lax.axis_size("gy")
    local = (mass, tracer, uvel, vvel, case_east, case_north)
    pairs = (ncat * ncomp + 4) // 2
    rows = height + 2 * PAD
    tall = FRONT + ncat * height + BACK
    block = FRONT + 32 * ncat + BACK
    deep = height + 3 * DEEP

    pay_a, pay_b, field, aux = call(
        pack_rows_kernel,
        tuple(pltpu.with_memory_space_constraint(x, pltpu.HBM) for x in (ice_blocks,) + local),
        (
            shape(pairs, 8, width),
            shape(pairs, 8, width),
            shape(ncomp, tall, width),
            shape(4, height + PAD, width),
        ),
        [
            pltpu.SMEM(ice_blocks.shape, jnp.int32),
            pltpu.VMEM((2, height, width), jnp.int32),
            pltpu.SemaphoreType.DMA((5 + 2 * ncat,)),
        ],
        1 << 20,
        specs=[HBM] * 7,
    )
    both = ("gx", "gy")
    pairs_a, pairs_b = [], []
    for j in range(ny):
        for i in range(nx):
            pairs_a.append((i * ny + j, i * ny + (j ^ 1)))
            if j == ny - 1:
                pairs_b.append((i * ny + j, (nx - 1 - i) * ny + j))
            elif j:
                pairs_b.append((i * ny + j, i * ny + (j + 1 if j % 2 else j - 1)))
    got_a = lax.ppermute(pay_a, both, pairs_a)
    got_b = lax.ppermute(pay_b, both, pairs_b)

    once, strips, geo = call(
        first_kernel,
        (field, aux),
        (shape(8, tall, width), shape(12, deep, width), shape(2, 7, rows, width)),
        [(8, 4, tall, width), (8, tall, width), (8, 8, width)],
        1 << 27,
    )
    halo, strips, pay_c, pay_d = call(
        pack_columns_kernel,
        (got_a, got_b, strips),
        (
            shape(2 * pairs, 16, width),
            shape(12, deep, width),
            shape(2, height + 2 * DEPTH, width),
            shape(2, height + 2 * DEPTH, width),
        ),
        [(2, pairs, 8, width), (pairs, 8, width)],
        1 << 20,
        aliases={2: 1},
    )
    got_c = lax.ppermute(pay_c, "gx", [(i, i ^ 1) for i in range(nx)])
    got_d = lax.ppermute(pay_d, "gx", [(i, (i + (1 if i % 2 else -1)) % nx) for i in range(nx)])
    (twice,) = call(
        second_kernel,
        (field, aux, once, geo, halo),
        (shape(8, tall, width),),
        [
            (2, 4, 40, width),
            (4, 40, width),
            (2, 2, 7, 40, width),
            (2, 7, 8, width),
            (8, block, width),
            (8, block, width),
            (8, 4, tall, width),
            (8, tall, width),
            (8, 8, width),
            (8, 8, width),
        ],
        1 << 27,
    )
    return call(
        finish_kernel,
        (strips, got_c, got_d, twice),
        (shape(ncat, height, width), shape(ncat, ncomp - 1, height, width)),
        [
            (2, 2, height + 2 * DEPTH, width),
            (12, deep, width),
            (4, 40, width),
            (2, 7, deep, width),
            (8, deep, width),
            (8, deep, width),
            (8, 4, deep, width),
            (8, deep, width),
            (8, 8, width),
            (ncat, 8, height, width),
            pltpu.SemaphoreType.DMA((2, ncat)),
        ],
        1 << 26,
        out_spec=HBM,
    )


def solution(mesh):
    placed = (
        P(None, "gy", "gx"),
        P(None, None, "gy", "gx"),
        P("gy", "gx"),
        P("gy", "gx"),
        P("gy", "gx"),
        P("gy", "gx"),
        P("gy", "gx"),
    )
    return jax.shard_map(
        per_device,
        mesh=mesh,
        in_specs=placed,
        out_specs=(P(None, "gy", "gx"), P(None, None, "gy", "gx")),
        check_vma=False,
    )
```
